128 devices in a mesh: wide: 32 (over z, x, core), head: 4 (over y).
Axes of the slice: x: 4, y: 4, z: 4, core: 2. Of those that a mesh axis runs over, the one named last changes fastest.
Arguments:
- queries: bfloat16 [16384, 8192], P(('wide', 'head')), may hold values from -6 to 6
- keys: bfloat16 [16384, 1024], P(('wide', 'head')), may hold values from -6 to 6
- values: bfloat16 [16384, 1024], P(('wide', 'head')), may hold values from -6 to 6
- out_rows: bfloat16 [16384, 8192], P(('wide', 'head')), may hold values from -3 to 3
- output_gradient: bfloat16 [16384, 8192], P(('wide', 'head')), may hold values from -3 to 3
- log_norm_rows: float32 [16384, 64], P(('wide', 'head')), may hold values from 4 to 8
- doc_lengths: int32 [16], replicated, may hold values from 1 to 1792, 16384 in all
Outputs:
- q_grad: float32 [16384, 8192], P(('wide', 'head'))
- key_gradient: float32 [16384, 1024], P(('wide', 'head'))
- value_gradient: float32 [16384, 1024], P(('wide', 'head'))
The draws below stay inside these ranges and needn't reach their ends.
Inputs may be any that keep to these rules, and one draw needn't show every extreme that they name: `doc_lengths`: 16 document lengths in order; they sum to 16384.
All inputs are finite; a program needn't handle non-finite values.
Results may differ from the reference program's by a relative error of at most 0.0058.
Values may be sent and summed in bfloat16 or wider, within the bound.
No kernel may reach another device: no remote copies, remote signals or barrier semaphores. Data moves between devices by JAX's collectives and lax.ppermute only.
A program may use at most 128 MiB of HBM per device.

```python
import math
import jax
import jax.numpy as jnp
import numpy as np
from jax import lax

QUERY_HEADS = 64
KEY_VALUE_HEADS = 8
HEAD_SIZE = 128
DOCS = 16
PACKED_TOKENS = 16384
DOC_MOST = 1792


def steps_of(rng, extent, shards, low, top_value):
    level = 1.0
    for axis_at, parts in shards:
        heights = jax.random.uniform(jax.random.fold_in(jax.random.fold_in(rng, 6), axis_at), (parts,), jnp.float32, low / len(shards), top_value / len(shards))
        level = level * jnp.repeat(jnp.exp(heights), extent[axis_at] // parts).reshape((-1,) + (1,) * (len(extent) - 1 - axis_at))
    return level


def split_up(number_of, total, limit, lean):
    weights = [(1 << 20) // math.isqrt(rank ** lean) + 1 for rank in range(2, number_of + 1)]
    rest, counts = total - limit - (number_of - 1), [1] * (number_of - 1)
    while rest > 0:
        movable = [i for i in range(number_of - 1) if counts[i] < limit]
        pool, left = sum([weights[i] for i in movable]), rest
        for i in movable:
            extra = min(limit - counts[i], max(1, left * weights[i] // pool), rest)
            counts[i] = counts[i] + extra
            rest = rest - extra
    return np.array([limit] + counts)


def uneven_parts(key, count, total, most, lean):
    if count == 2:
        one = jax.random.randint(key, (), max(1, total - most), min(most, total - 1) + 1)
        return jnp.stack([one, total - one])
    lengths = jnp.asarray(split_up(count, total, most, lean), jnp.int32)
    twos = (count - 1) // 2
    source_of, sink = lengths[1:1 + 2 * twos:2], lengths[2:2 + 2 * twos:2]
    margin = jnp.minimum(source_of - 1, most - sink)
    shifted = jax.random.randint(jax.random.fold_in(key, 1), (twos,), 0, 1 << 20) % (margin + 1)
    lengths = lengths.at[1:1 + 2 * twos:2].set(source_of - shifted).at[2:2 + 2 * twos:2].set(sink + shifted)
    return lengths[jax.random.permutation(jax.random.fold_in(key, 2), count)]


def normal_values(rng, extent, width, most, shards=(), kind=jnp.bfloat16):
    values = width * jax.random.normal(rng, extent, jnp.float32)
    if shards:
        values = values * steps_of(rng, extent, shards, -0.22, 0.18)
    return jnp.clip(values, -most, most).astype(kind)


def setup_inputs(seed: int = 0) -> dict:
    key_list = jax.random.split(jax.random.key(seed), 8)
    queries = normal_values(key_list[0], (PACKED_TOKENS, QUERY_HEADS * HEAD_SIZE), 1.0, 6.0, ((0, 128),))
    keys = normal_values(key_list[1], (PACKED_TOKENS, KEY_VALUE_HEADS * HEAD_SIZE), 1.0, 6.0, ((0, 128),))
    values = normal_values(key_list[2], (PACKED_TOKENS, KEY_VALUE_HEADS * HEAD_SIZE), 1.0, 6.0, ((0, 128),))
    out_rows = normal_values(key_list[3], (PACKED_TOKENS, QUERY_HEADS * HEAD_SIZE), 0.5, 3.0, ((0, 128),))
    output_gradient = normal_values(key_list[4], (PACKED_TOKENS, QUERY_HEADS * HEAD_SIZE), 0.5, 3.0, ((0, 128),))
    log_norm_rows = jnp.clip(4.0 + 4.0 * jax.random.uniform(key_list[5], (PACKED_TOKENS, QUERY_HEADS), jnp.float32) ** steps_of(key_list[5], (PACKED_TOKENS, QUERY_HEADS), ((0, 128),), -0.2, 0.2), 4.0, 8.0)
    doc_lengths = uneven_parts(key_list[6], DOCS, PACKED_TOKENS, DOC_MOST, 2).astype(jnp.int32)
    return dict(queries=queries, keys=keys, values=values, out_rows=out_rows, output_gradient=output_gradient, log_norm_rows=log_norm_rows, doc_lengths=doc_lengths)


def doc_number(doc_lengths, positions):
    doc_ends = jnp.cumsum(doc_lengths)
    found = lax.optimization_barrier(jnp.sum((doc_ends[None, :] <= positions[:, None]).astype(jnp.int32), axis=1))
    return jnp.where(positions < 0, -1, found).astype(jnp.int32)

def pair_terms(query_rows, grad_rows, norm_rows, delta_rows, allowed, k_block, v_block, scaling):
    row_count = allowed.shape[0]
    key_count = k_block.shape[0]
    group_count = norm_rows.shape[1]
    forward_dims = (((1,), (1,)), ((), ()))
    backward_dims = (((0,), (0,)), ((), ()))
    scores = lax.dot_general(query_rows, k_block, forward_dims, preferred_element_type=jnp.float32)
    scores = scores.reshape(row_count, group_count, key_count)
    attend = jnp.where(allowed[:, None, :], jnp.exp(scores * scaling - norm_rows[:, :, None]), 0.0)
    prob_grad = lax.dot_general(grad_rows, v_block, forward_dims, preferred_element_type=jnp.float32)
    prob_grad = prob_grad.reshape(row_count, group_count, key_count)
    score_grad = attend * (prob_grad - delta_rows[:, :, None])
    attend_low = attend.astype(jnp.bfloat16).reshape(row_count * group_count, key_count)
    score_low = score_grad.astype(jnp.bfloat16).reshape(row_count * group_count, key_count)
    value_term = lax.dot_general(attend_low, grad_rows, backward_dims, preferred_element_type=jnp.float32)
    key_term = lax.dot_general(score_low, query_rows, backward_dims, preferred_element_type=jnp.float32)
    query_term = jnp.dot(score_low, k_block, preferred_element_type=jnp.float32)
    return (query_term, key_term, value_term)

def reference(queries, keys, values, out_rows, output_gradient, log_norm_rows, doc_lengths):
    every_row_set = queries.shape[0]
    group_count = QUERY_HEADS // KEY_VALUE_HEADS
    scaling = 1.0 / math.sqrt(HEAD_SIZE)
    delta_per_row = lax.optimization_barrier(jnp.sum((output_gradient.astype(jnp.float32) * out_rows.astype(jnp.float32)).reshape(every_row_set, QUERY_HEADS, HEAD_SIZE), axis=2))
    tile_rows = min(256, every_row_set)
    tile_count = every_row_set // tile_rows
    positions = jnp.arange(every_row_set, dtype=jnp.int32)
    doc_index = doc_number(doc_lengths, positions)
    query_per_head = queries.reshape(every_row_set, KEY_VALUE_HEADS, group_count * HEAD_SIZE).transpose(1, 0, 2)
    gradient_per_head = output_gradient.reshape(every_row_set, KEY_VALUE_HEADS, group_count * HEAD_SIZE).transpose(1, 0, 2)
    norm_per_head = log_norm_rows.reshape(every_row_set, KEY_VALUE_HEADS, group_count).transpose(1, 0, 2)
    delta_per_head = delta_per_row.reshape(every_row_set, KEY_VALUE_HEADS, group_count).transpose(1, 0, 2)
    key_per_head = keys.reshape(every_row_set, KEY_VALUE_HEADS, HEAD_SIZE).transpose(1, 0, 2)
    value_per_head = values.reshape(every_row_set, KEY_VALUE_HEADS, HEAD_SIZE).transpose(1, 0, 2)

    def one_head(operands):
        query_head, grad_head, norm_head, delta_head, key_head, value_head = operands

        def visit(pair_index, running):
            query_tile = (pair_index // tile_count).astype(jnp.int32)
            key_tile = (pair_index % tile_count).astype(jnp.int32)
            query_start = (query_tile * tile_rows).astype(jnp.int32)
            key_start = (key_tile * tile_rows).astype(jnp.int32)
            needed = (key_tile <= query_tile) & (doc_index[key_start + tile_rows - 1] >= doc_index[query_start])

            def compute(state):
                query_acc, key_acc, value_acc = state
                query_rows = lax.dynamic_slice_in_dim(query_head, query_start, tile_rows, 0).reshape(tile_rows * group_count, HEAD_SIZE)
                grad_rows = lax.dynamic_slice_in_dim(grad_head, query_start, tile_rows, 0).reshape(tile_rows * group_count, HEAD_SIZE)
                norm_rows = lax.dynamic_slice_in_dim(norm_head, query_start, tile_rows, 0)
                delta_rows = lax.dynamic_slice_in_dim(delta_head, query_start, tile_rows, 0)
                k_block = lax.dynamic_slice_in_dim(key_head, key_start, tile_rows, 0)
                v_block = lax.dynamic_slice_in_dim(value_head, key_start, tile_rows, 0)
                query_pos = lax.dynamic_slice_in_dim(positions, query_start, tile_rows, 0)
                key_pos = lax.dynamic_slice_in_dim(positions, key_start, tile_rows, 0)
                query_doc = lax.dynamic_slice_in_dim(doc_index, query_start, tile_rows, 0)
                key_doc = lax.dynamic_slice_in_dim(doc_index, key_start, tile_rows, 0)
                allowed = (query_doc[:, None] == key_doc[None, :]) & (key_pos[None, :] <= query_pos[:, None])
                query_term, key_term, value_term = pair_terms(query_rows, grad_rows, norm_rows, delta_rows, allowed, k_block, v_block, scaling)
                query_old = lax.dynamic_slice_in_dim(query_acc, query_start, tile_rows, 0)
                query_acc = lax.dynamic_update_slice_in_dim(query_acc, query_old + query_term.reshape(tile_rows, group_count * HEAD_SIZE), query_start, 0)
                key_old = lax.dynamic_slice_in_dim(key_acc, key_start, tile_rows, 0)
                key_acc = lax.dynamic_update_slice_in_dim(key_acc, key_old + key_term, key_start, 0)
                value_old = lax.dynamic_slice_in_dim(value_acc, key_start, tile_rows, 0)
                value_acc = lax.dynamic_update_slice_in_dim(value_acc, value_old + value_term, key_start, 0)
                return (query_acc, key_acc, value_acc)

            def skipped(state):
                return state
            return lax.cond(needed, compute, skipped, running)
        initial = (jnp.zeros((every_row_set, group_count * HEAD_SIZE), jnp.float32), jnp.zeros((every_row_set, HEAD_SIZE), jnp.float32), jnp.zeros((every_row_set, HEAD_SIZE), jnp.float32))
        query_acc, key_acc, value_acc = lax.fori_loop(0, tile_count * tile_count, visit, initial)
        return (query_acc * scaling, key_acc * scaling, value_acc)
    query_all, key_everything, value_everything = lax.map(one_head, (query_per_head, gradient_per_head, norm_per_head, delta_per_head, key_per_head, value_per_head))
    q_grad = query_all.transpose(1, 0, 2).reshape(every_row_set, QUERY_HEADS * HEAD_SIZE)
    key_gradient = key_everything.transpose(1, 0, 2).reshape(every_row_set, KEY_VALUE_HEADS * HEAD_SIZE)
    value_gradient = value_everything.transpose(1, 0, 2).reshape(every_row_set, KEY_VALUE_HEADS * HEAD_SIZE)
    return (q_grad, key_gradient, value_gradient)
```

```python
import math

import jax
import jax.numpy as jnp
from jax import lax
from jax.experimental import pallas as pl
from jax.experimental.pallas import tpu as pltpu
from jax.sharding import Mesh, PartitionSpec as P

LOG2E = math.log2(math.e)
HEAD = 128
ROWS = 128
MEMBERS = 8
GROUP = MEMBERS * ROWS
FAR_BLOCKS = 14
FAR = FAR_BLOCKS * ROWS
FAR2 = FAR - GROUP
WINDOW = FAR + GROUP
HEADS = 8
CHUNKS = 2
H = HEADS // CHUNKS
TQ = 256
TK = 256
NT = (((1,), (1,)), ((), ()))
TN = (((0,), (0,)), ((), ()))

SMEM = pl.BlockSpec(memory_space=pltpu.SMEM)
VMEM = pl.BlockSpec(memory_space=pltpu.VMEM)
BIG = pltpu.CompilerParams(vmem_limit_bytes=56 << 20)


def kv_pack(keys, values):
    def kernel(k_ref, v_ref, out_ref):
        for b in range(MEMBERS):
            out_ref[b, :, 0:HEAD] = k_ref[:, b * HEAD : (b + 1) * HEAD]
            out_ref[b, :, HEAD : 2 * HEAD] = v_ref[:, b * HEAD : (b + 1) * HEAD]

    return pl.pallas_call(
        kernel,
        in_specs=[VMEM, VMEM],
        out_specs=VMEM,
        out_shape=jax.ShapeDtypeStruct((MEMBERS, ROWS, 2 * HEAD), jnp.bfloat16),
        name="kv_pack",
    )(keys, values)


def rows_pack(queries, grads, chunk):
    width = H * HEAD

    def kernel(q_ref, g_ref, out_ref):
        out_ref[0, :, 0:width] = q_ref[...]
        out_ref[0, :, width : 2 * width] = g_ref[...]

    source = pl.BlockSpec((ROWS, width), lambda b: (0, b * CHUNKS + chunk))
    return pl.pallas_call(
        kernel,
        grid=(MEMBERS,),
        in_specs=[source, source],
        out_specs=pl.BlockSpec((1, ROWS, 2 * width), lambda b: (b, 0, 0)),
        out_shape=jax.ShapeDtypeStruct((MEMBERS, ROWS, 2 * width), jnp.bfloat16),
        name="rows_pack",
    )(queries, grads)


def stats_pack(grads, outs, norms):
    def kernel(g_ref, o_ref, n_ref, out_ref, turned):
        b = pl.program_id(0)

        @pl.when(b == 0)
        def _():
            turned[...] = n_ref[...].T

        lane = lax.broadcasted_iota(jnp.int32, (ROWS, 128), 1)
        deltas = jnp.zeros((ROWS, 128), jnp.float32)
        for h in range(HEADS):
            cut = slice(h * HEAD, (h + 1) * HEAD)
            product = g_ref[:, cut].astype(jnp.float32) * o_ref[:, cut].astype(jnp.float32)
            deltas = jnp.where(lane == h, jnp.sum(product, axis=1, keepdims=True), deltas)
        out_ref[0, 0:HEADS, :] = turned[pl.ds(pl.multiple_of(b * HEADS, HEADS), HEADS), :]
        out_ref[0, HEADS : 2 * HEADS, :] = deltas.T[0:HEADS]

    source = pl.BlockSpec((ROWS, HEADS * HEAD), lambda b: (0, b))
    return pl.pallas_call(
        kernel,
        grid=(MEMBERS,),
        in_specs=[source, source, pl.BlockSpec(norms.shape, lambda b: (0, 0))],
        out_specs=pl.BlockSpec((1, 2 * HEADS, ROWS), lambda b: (b, 0, 0)),
        out_shape=jax.ShapeDtypeStruct((MEMBERS, 2 * HEADS, ROWS), jnp.float32),
        scratch_shapes=[pltpu.VMEM((norms.shape[1], ROWS), jnp.float32)],
        name="stats_pack",
    )(grads, outs, norms)


def attention(starts, first_token, rows, stats, far2, far1, near, sums, chunk):
    scaling = 1.0 / math.sqrt(HEAD)
    docs = starts.shape[0]
    parts = TQ // ROWS
    last = chunk == CHUNKS - 1

    def kernel(starts_ref, first_ref, rows_ref, stats_ref, far2_ref, far1_ref, near_ref, *rest):
        if sums is not None:
            sums_ref, *rest = rest
        if last:
            q_out, far2_out, far1_out, near_out, window, acc, q_acc = rest
        else:
            q_out, acc, window, q_acc = rest
        window[0:FAR2] = far2_ref[...]
        window[FAR2:FAR] = far1_ref[...]
        window[FAR:WINDOW] = near_ref[...]
        if sums is not None:
            acc[...] = sums_ref[...]
        else:
            acc[...] = jnp.zeros_like(acc)
        group_first = first_ref[0]
        window_first = group_first - FAR

        def query_tile(tile, carry):
            token = group_first + tile * TQ
            doc_first = lax.fori_loop(
                0, docs, lambda i, m: jnp.where(starts_ref[i] <= token, starts_ref[i], m), jnp.int32(0)
            )
            position = token + lax.broadcasted_iota(jnp.int32, (8, TQ), 1)
            doc_start = lax.fori_loop(
                0,
                docs,
                lambda i, m: jnp.where(position >= starts_ref[i], starts_ref[i], m),
                jnp.zeros((8, TQ), jnp.int32),
            )
            low = doc_start[0:1] - window_first
            reach = position[0:1] - doc_start[0:1]
            key_begin = (doc_first - window_first) // TK
            key_end = (token + TQ - 1 - window_first) // TK + 1
            block = tile * parts
            pairs = [(h, s) for h in range(H) for s in range(parts)]
            query = jnp.concatenate(
                [rows_ref[block + s, :, h * HEAD : (h + 1) * HEAD] for h, s in pairs], axis=0
            )
            grad = jnp.concatenate(
                [rows_ref[block + s, :, (H + h) * HEAD : (H + h + 1) * HEAD] for h, s in pairs],
                axis=0,
            )
            at = chunk * H
            norm = LOG2E * jnp.concatenate(
                [stats_ref[block + s, at + h : at + h + 1, :] for h, s in pairs], axis=1
            )
            delta = jnp.concatenate(
                [stats_ref[block + s, HEADS + at + h : HEADS + at + h + 1, :] for h, s in pairs],
                axis=1,
            )
            q_acc[...] = jnp.zeros_like(q_acc)

            def key_tile(index, inner):
                row = pl.multiple_of(index * TK, TK)
                k_rows = window[pl.ds(row, TK), 0:HEAD]
                v_rows = window[pl.ds(row, TK), HEAD : 2 * HEAD]
                offset = row + lax.broadcasted_iota(jnp.int32, (TK, TQ), 0) - low
                allowed = (offset >= 0) & (offset <= reach)
                allowed = jnp.concatenate([allowed] * H, axis=1)
                scores = lax.dot_general(k_rows, query, NT, preferred_element_type=jnp.float32)
                attend = jnp.where(allowed, jnp.exp2(scores * (scaling * LOG2E) - norm), 0.0)
                prob_grad = lax.dot_general(v_rows, grad, NT, preferred_element_type=jnp.float32)
                score_low = (attend * (prob_grad - delta)).astype(jnp.bfloat16)
                attend_low = attend.astype(jnp.bfloat16)
                acc[pl.ds(row, TK), HEAD : 2 * HEAD] += jnp.dot(
                    attend_low, grad, preferred_element_type=jnp.float32
                )
                acc[pl.ds(row, TK), 0:HEAD] += jnp.dot(
                    score_low, query, preferred_element_type=jnp.float32
                )
                q_acc[...] += lax.dot_general(
                    score_low, k_rows, TN, preferred_element_type=jnp.float32
                )
                return inner

            lax.fori_loop(key_begin, key_end, key_tile, 0)
            for at_row, (h, s) in enumerate(pairs):
                part = q_acc[at_row * ROWS : (at_row + 1) * ROWS, :] * scaling
                q_out[block + s, :, h * HEAD : (h + 1) * HEAD] = part.astype(jnp.bfloat16)
            return carry

        lax.fori_loop(0, GROUP // TQ, query_tile, 0)
        if last:
            for ref, begin, end in (
                (far2_out, 0, FAR2),
                (far1_out, FAR2, FAR),
                (near_out, FAR, WINDOW),
            ):
                ref[:, 0:HEAD] = (acc[begin:end, 0:HEAD] * scaling).astype(ref.dtype)
                ref[:, HEAD : 2 * HEAD] = acc[begin:end, HEAD : 2 * HEAD].astype(ref.dtype)

    pair = 2 * HEAD
    q_shape = jax.ShapeDtypeStruct((MEMBERS, ROWS, H * HEAD), jnp.bfloat16)
    acc_shape = (WINDOW, pair)
    window_scratch = pltpu.VMEM((WINDOW, pair), jnp.bfloat16)
    q_scratch = pltpu.VMEM((H * TQ, HEAD), jnp.float32)
    if last:
        out_shape = [
            q_shape,
            jax.ShapeDtypeStruct((FAR2, pair), jnp.bfloat16),
            jax.ShapeDtypeStruct((GROUP, pair), jnp.bfloat16),
            jax.ShapeDtypeStruct((GROUP, pair), jnp.float32),
        ]
        scratch = [window_scratch, pltpu.VMEM(acc_shape, jnp.float32), q_scratch]
    else:
        out_shape = [q_shape, jax.ShapeDtypeStruct(acc_shape, jnp.float32)]
        scratch = [window_scratch, q_scratch]
    operands = [starts, first_token, rows, stats, far2, far1, near]
    if sums is not None:
        operands.append(sums)
    return pl.pallas_call(
        kernel,
        in_specs=[SMEM, SMEM] + [VMEM] * (len(operands) - 2),
        out_specs=[VMEM] * len(out_shape),
        out_shape=out_shape,
        scratch_shapes=scratch,
        compiler_params=BIG,
        name=f"attention_{chunk}",
    )(*operands)


def kv_sum(near, back1, back2):
    def kernel(near_ref, back1_ref, back2_ref, out_ref):
        for b in range(MEMBERS):
            cut = slice(b * ROWS, (b + 1) * ROWS)
            total = near_ref[cut] + back1_ref[cut].astype(jnp.float32)
            skip = (GROUP - FAR2) // ROWS
            if b >= skip:
                far = slice((b - skip) * ROWS, (b - skip + 1) * ROWS)
                total = total + back2_ref[far].astype(jnp.float32)
            out_ref[b] = total.astype(jnp.bfloat16)

    return pl.pallas_call(
        kernel,
        in_specs=[VMEM] * 3,
        out_specs=VMEM,
        out_shape=jax.ShapeDtypeStruct((MEMBERS, ROWS, 2 * HEAD), jnp.bfloat16),
        name="kv_sum",
    )(near, back1, back2)


def q_unpack(parts):
    width = H * HEAD

    def kernel(*refs):
        for chunk in range(CHUNKS):
            refs[-1][:, chunk * width : (chunk + 1) * width] = refs[chunk][0].astype(jnp.float32)

    return pl.pallas_call(
        kernel,
        grid=(MEMBERS,),
        in_specs=[pl.BlockSpec((1, ROWS, width), lambda b: (b, 0, 0))] * CHUNKS,
        out_specs=pl.BlockSpec((ROWS, CHUNKS * width), lambda b: (0, b)),
        out_shape=jax.ShapeDtypeStruct((ROWS, MEMBERS * CHUNKS * width), jnp.float32),
        name="q_unpack",
    )(*parts)


def kv_unpack(both):
    def kernel(both_ref, k_ref, v_ref):
        for b in range(MEMBERS):
            k_ref[:, b * HEAD : (b + 1) * HEAD] = both_ref[b, :, 0:HEAD].astype(jnp.float32)
            v_ref[:, b * HEAD : (b + 1) * HEAD] = both_ref[b, :, HEAD:].astype(jnp.float32)

    shape = jax.ShapeDtypeStruct((ROWS, MEMBERS * HEAD), jnp.float32)
    return pl.pallas_call(
        kernel,
        in_specs=[VMEM],
        out_specs=[VMEM, VMEM],
        out_shape=[shape, shape],
        name="kv_unpack",
    )(both)


def exchange(blocks):
    return lax.all_to_all(blocks, ("core", "head"), split_axis=0, concat_axis=0, tiled=True)


def shifted(block, by):
    count = lax.axis_size("group")
    pairs = [(i, i + by) for i in range(count) if 0 <= i + by < count]
    return lax.ppermute(block, "group", pairs)


def on_device(queries, keys, values, out_rows, output_gradient, log_norm_rows, doc_lengths):
    near = exchange(kv_pack(keys, values)).reshape(GROUP, 2 * HEAD)
    rows = [exchange(rows_pack(queries, output_gradient, chunk)) for chunk in range(CHUNKS)]
    stats = exchange(stats_pack(output_gradient, out_rows, log_norm_rows))
    far1 = shifted(near, 1)
    far2 = shifted(near[GROUP - FAR2 :], 2)
    starts = jnp.cumsum(doc_lengths) - doc_lengths
    first_token = (lax.axis_index("group") * GROUP).astype(jnp.int32).reshape(1)
    sums = None
    q_parts = []
    for chunk in range(CHUNKS):
        q_part, *sums_out = attention(
            starts, first_token, rows[chunk], stats, far2, far1, near, sums, chunk
        )
        q_parts.append(exchange(q_part))
        sums = sums_out[0]
    far2_sum, far1_sum, near_sum = sums_out
    both = kv_sum(near_sum, shifted(far1_sum, -1), shifted(far2_sum, -2))
    key_gradient, value_gradient = kv_unpack(exchange(both))
    return (q_unpack(q_parts), key_gradient, value_gradient)


def solution(mesh):
    wide, head = mesh.shape["wide"], mesh.shape["head"]
    cores = MEMBERS // head
    finer = Mesh(mesh.devices.reshape(wide // cores, cores, head), ("group", "core", "head"))
    split = P(("group", "core", "head"), None)
    return jax.shard_map(
        on_device,
        mesh=finer,
        in_specs=(split,) * 6 + (P(),),
        out_specs=(split, split, split),
        check_vma=False,
    )
```

```python
import math

import jax
import jax.numpy as jnp
from jax import lax
from jax.experimental import pallas as pl
from jax.experimental.pallas import tpu as pltpu
from jax.sharding import Mesh, PartitionSpec as P


LOG2E = math.log2(math.e)
HEAD = 128
ROWS = 128
MEMBERS = 8
GROUP = MEMBERS * ROWS
FAR_BLOCKS = 14
FAR = FAR_BLOCKS * ROWS
FAR2 = FAR - GROUP
WINDOW = FAR + GROUP
HEADS = 8
CHUNKS = 2
H = HEADS // CHUNKS
WIDTH = H * HEAD
STATS = 2 * H
TQ = 256
TK = 256
NT = (((1,), (1,)), ((), ()))
TN = (((0,), (0,)), ((), ()))

SMEM = pl.BlockSpec(memory_space=pltpu.SMEM)
VMEM = pl.BlockSpec(memory_space=pltpu.VMEM)
ANY = pl.BlockSpec(memory_space=pl.ANY)
BIG = pltpu.CompilerParams(vmem_limit_bytes=56 << 20)


def kv_pack(keys, values):
    def kernel(k_ref, v_ref, out_ref):
        for b in range(MEMBERS):
            out_ref[b, :, 0:HEAD] = k_ref[:, b * HEAD : (b + 1) * HEAD]
            out_ref[b, :, HEAD : 2 * HEAD] = v_ref[:, b * HEAD : (b + 1) * HEAD]

    return pl.pallas_call(
        kernel,
        in_specs=[VMEM, VMEM],
        out_specs=VMEM,
        out_shape=jax.ShapeDtypeStruct((MEMBERS, ROWS, 2 * HEAD), jnp.bfloat16),
        name="kv_pack",
    )(keys, values)


def split_terms(value):
    high = value.astype(jnp.bfloat16)
    rest = value - high.astype(jnp.float32)
    middle = rest.astype(jnp.bfloat16)
    low = (rest - middle.astype(jnp.float32)).astype(jnp.bfloat16)
    return high, middle, low


def rows_pack(queries, grads, outs, norms, chunk):
    def kernel(q_ref, g_ref, o_ref, n_ref, out_ref, packed, forward, arrived, sent):
        def inbound(b):
            cut = pl.ds((b * CHUNKS + chunk) * WIDTH, WIDTH)
            return (
                pltpu.make_async_copy(
                    q_ref.at[:, cut], packed.at[b, pl.ds(0, ROWS), pl.ds(0, WIDTH)], arrived.at[0, b]
                ),
                pltpu.make_async_copy(
                    g_ref.at[:, cut],
                    packed.at[b, pl.ds(0, ROWS), pl.ds(WIDTH, WIDTH)],
                    arrived.at[1, b],
                ),
                pltpu.make_async_copy(o_ref.at[:, cut], forward.at[b], arrived.at[2, b]),
            )

        for b in range(MEMBERS):
            for copy in inbound(b):
                copy.start()
        lane = lax.broadcasted_iota(jnp.int32, (ROWS, 128), 1)
        for b in range(MEMBERS):
            for copy in inbound(b):
                copy.wait()
            deltas = jnp.zeros((ROWS, 128), jnp.float32)
            for h in range(H):
                cut = slice(h * HEAD, (h + 1) * HEAD)
                grad = packed[b, 0:ROWS, WIDTH + h * HEAD : WIDTH + (h + 1) * HEAD]
                product = grad.astype(jnp.float32) * forward[b, :, cut].astype(jnp.float32)
                deltas = jnp.where(lane == h, jnp.sum(product, axis=1, keepdims=True), deltas)
            first = b * HEADS + chunk * H
            stats = jnp.concatenate([n_ref[first : first + H], deltas.T[0:H]], axis=0)
            high, middle, low = split_terms(stats)
            packed[b, ROWS : ROWS + STATS, 0:ROWS] = high
            packed[b, ROWS : ROWS + STATS, ROWS : 2 * ROWS] = middle
            packed[b, ROWS : ROWS + STATS, 2 * ROWS : 3 * ROWS] = low
            packed[b, ROWS : ROWS + STATS, 3 * ROWS :] = jnp.zeros(
                (STATS, 2 * WIDTH - 3 * ROWS), jnp.bfloat16
            )
            pltpu.make_async_copy(packed.at[b], out_ref.at[b], sent.at[b]).start()
        for b in range(MEMBERS):
            pltpu.make_async_copy(packed.at[b], out_ref.at[b], sent.at[b]).wait()

    shape = (MEMBERS, ROWS + STATS, 2 * WIDTH)
    return pl.pallas_call(
        kernel,
        in_specs=[ANY, ANY, ANY, VMEM],
        out_specs=ANY,
        out_shape=jax.ShapeDtypeStruct(shape, jnp.bfloat16),
        scratch_shapes=[
            pltpu.VMEM(shape, jnp.bfloat16),
            pltpu.VMEM((MEMBERS, ROWS, WIDTH), jnp.bfloat16),
            pltpu.SemaphoreType.DMA((3, MEMBERS)),
            pltpu.SemaphoreType.DMA((MEMBERS,)),
        ],
        compiler_params=BIG,
        name="rows_pack",
    )(queries, grads, outs, norms)


def relay(block):
    def kernel(block_ref, out_ref, copied):
        copy = pltpu.make_async_copy(block_ref.at[pl.ds(GROUP - FAR2, FAR2)], out_ref, copied)
        copy.start()
        copy.wait()

    return pl.pallas_call(
        kernel,
        in_specs=[ANY],
        out_specs=ANY,
        out_shape=jax.ShapeDtypeStruct((FAR2, 2 * HEAD), jnp.bfloat16),
        scratch_shapes=[pltpu.SemaphoreType.DMA],
        name="relay",
    )(block)


def attention(doc_lengths, first_token, rows, far2, far1, near, earlier, chunk):
    scaling = 1.0 / math.sqrt(HEAD)
    docs = doc_lengths.shape[0]
    parts = TQ // ROWS
    last = chunk == CHUNKS - 1
    q_at = chunk * WIDTH if last else 0

    def kernel(lengths_ref, first_ref, rows_ref, far2_ref, far1_ref, near_ref, *rest):
        if last:
            q_earlier, sums_ref, q_out, far2_out, far1_out, near_out, window, acc, q_acc = rest
        else:
            q_out, acc, window, q_acc = rest
        window[0:FAR2] = far2_ref[...]
        window[FAR2:FAR] = far1_ref[...]
        window[FAR:WINDOW] = near_ref[...]
        if last:
            acc[...] = sums_ref[...]
            q_out[:, :, 0 : chunk * WIDTH] = q_earlier[...]
        else:
            acc[...] = jnp.zeros_like(acc)
        group_first = first_ref[0]
        window_first = group_first - FAR

        def query_tile(tile, carry):
            token = group_first + tile * TQ
            position = token + lax.broadcasted_iota(jnp.int32, (8, TQ), 1)
            start = jnp.int32(0)
            doc_first = start
            doc_start = jnp.zeros((8, TQ), jnp.int32)
            for doc in range(1, docs):
                start = start + lengths_ref[doc - 1]
                doc_first = jnp.where(start <= token, start, doc_first)
                doc_start = jnp.where(start <= position, start, doc_start)
            low = doc_start[0:1] - window_first
            reach = position[0:1] - doc_start[0:1]
            key_begin = (doc_first - window_first) // TK
            key_end = (token + TQ - 1 - window_first) // TK + 1
            block = tile * parts
            pairs = [(h, s) for h in range(H) for s in range(parts)]
            query = jnp.concatenate(
                [rows_ref[block + s, 0:ROWS, h * HEAD : (h + 1) * HEAD] for h, s in pairs], axis=0
            )
            grad = jnp.concatenate(
                [rows_ref[block + s, 0:ROWS, WIDTH + h * HEAD : WIDTH + (h + 1) * HEAD] for h, s in pairs],
                axis=0,
            )
            stats = [
                sum(
                    rows_ref[block + s, ROWS : ROWS + STATS, t * ROWS : (t + 1) * ROWS].astype(
                        jnp.float32
                    )
                    for t in (2, 1, 0)
                )
                for s in range(parts)
            ]
            norm = LOG2E * jnp.concatenate([stats[s][h : h + 1] for h, s in pairs], axis=1)
            delta = jnp.concatenate([stats[s][H + h : H + h + 1] for h, s in pairs], axis=1)
            q_acc[...] = jnp.zeros_like(q_acc)

            def key_tile(index, inner):
                row = pl.multiple_of(index * TK, TK)
                k_rows = window[pl.ds(row, TK), 0:HEAD]
                v_rows = window[pl.ds(row, TK), HEAD : 2 * HEAD]
                offset = row + lax.broadcasted_iota(jnp.int32, (TK, TQ), 0) - low
                allowed = (offset >= 0) & (offset <= reach)
                allowed = jnp.concatenate([allowed] * H, axis=1)
                scores = lax.dot_general(k_rows, query, NT, preferred_element_type=jnp.float32)
                attend = jnp.where(allowed, jnp.exp2(scores * (scaling * LOG2E) - norm), 0.0)
                prob_grad = lax.dot_general(v_rows, grad, NT, preferred_element_type=jnp.float32)
                score_low = (attend * (prob_grad - delta)).astype(jnp.bfloat16)
                attend_low = attend.astype(jnp.bfloat16)
                acc[pl.ds(row, TK), HEAD : 2 * HEAD] += jnp.dot(
                    attend_low, grad, preferred_element_type=jnp.float32
                )
                acc[pl.ds(row, TK), 0:HEAD] += jnp.dot(
                    score_low, query, preferred_element_type=jnp.float32
                )
                q_acc[...] += lax.dot_general(
                    score_low, k_rows, TN, preferred_element_type=jnp.float32
                )
                return inner

            lax.fori_loop(key_begin, key_end, key_tile, 0)
            for at_row, (h, s) in enumerate(pairs):
                part = q_acc[at_row * ROWS : (at_row + 1) * ROWS, :] * scaling
                q_out[block + s, :, q_at + h * HEAD : q_at + (h + 1) * HEAD] = part.astype(
                    jnp.bfloat16
                )
            return carry

        lax.fori_loop(0, GROUP // TQ, query_tile, 0)
        if last:
            for ref, begin, end in (
                (far2_out, 0, FAR2),
                (far1_out, FAR2, FAR),
                (near_out, FAR, WINDOW),
            ):
                ref[:, 0:HEAD] = (acc[begin:end, 0:HEAD] * scaling).astype(ref.dtype)
                ref[:, HEAD : 2 * HEAD] = acc[begin:end, HEAD : 2 * HEAD].astype(ref.dtype)

    pair = 2 * HEAD
    q_shape = jax.ShapeDtypeStruct((MEMBERS, ROWS, q_at + WIDTH), jnp.bfloat16)
    acc_shape = (WINDOW, pair)
    window_scratch = pltpu.VMEM((WINDOW, pair), jnp.bfloat16)
    q_scratch = pltpu.VMEM((H * TQ, HEAD), jnp.float32)
    if last:
        out_shape = [
            q_shape,
            jax.ShapeDtypeStruct((FAR2, pair), jnp.bfloat16),
            jax.ShapeDtypeStruct((GROUP, pair), jnp.bfloat16),
            jax.ShapeDtypeStruct((GROUP, pair), jnp.float32),
        ]
        scratch = [window_scratch, pltpu.VMEM(acc_shape, jnp.float32), q_scratch]
    else:
        out_shape = [q_shape, jax.ShapeDtypeStruct(acc_shape, jnp.float32)]
        scratch = [window_scratch, q_scratch]
    operands = [doc_lengths, first_token, rows, far2, far1, near, *earlier]
    return pl.pallas_call(
        kernel,
        in_specs=[SMEM, SMEM] + [VMEM] * (len(operands) - 2),
        out_specs=[VMEM] * len(out_shape),
        out_shape=out_shape,
        scratch_shapes=scratch,
        compiler_params=BIG,
    )(*operands)


def kv_sum(near, back1, back2):
    def kernel(near_ref, back1_ref, back2_ref, out_ref):
        for b in range(MEMBERS):
            cut = slice(b * ROWS, (b + 1) * ROWS)
            total = near_ref[cut] + back1_ref[cut].astype(jnp.float32)
            skip = (GROUP - FAR2) // ROWS
            if b >= skip:
                far = slice((b - skip) * ROWS, (b - skip + 1) * ROWS)
                total = total + back2_ref[far].astype(jnp.float32)
            out_ref[b] = total.astype(jnp.bfloat16)

    return pl.pallas_call(
        kernel,
        in_specs=[VMEM] * 3,
        out_specs=VMEM,
        out_shape=jax.ShapeDtypeStruct((MEMBERS, ROWS, 2 * HEAD), jnp.bfloat16),
        name="kv_sum",
    )(near, back1, back2)


def q_unpack(blocks):
    width = HEADS * HEAD

    def kernel(in_ref, out_ref, narrow, wide, arrived, sent):
        def inbound(b):
            return pltpu.make_async_copy(in_ref.at[b], narrow.at[b], arrived.at[b])

        def outbound(b):
            return pltpu.make_async_copy(
                wide.at[b], out_ref.at[:, pl.ds(b * width, width)], sent.at[b]
            )

        for b in range(MEMBERS):
            inbound(b).start()
        for b in range(MEMBERS):
            inbound(b).wait()
            wide[b] = narrow[b].astype(jnp.float32)
            outbound(b).start()
        for b in range(MEMBERS):
            outbound(b).wait()

    shape = (MEMBERS, ROWS, width)
    return pl.pallas_call(
        kernel,
        in_specs=[ANY],
        out_specs=ANY,
        out_shape=jax.ShapeDtypeStruct((ROWS, MEMBERS * width), jnp.float32),
        scratch_shapes=[
            pltpu.VMEM(shape, jnp.bfloat16),
            pltpu.VMEM(shape, jnp.float32),
            pltpu.SemaphoreType.DMA((MEMBERS,)),
            pltpu.SemaphoreType.DMA((MEMBERS,)),
        ],
        compiler_params=BIG,
        name="q_unpack",
    )(blocks)


def kv_unpack(both):
    def kernel(both_ref, k_ref, v_ref):
        for b in range(MEMBERS):
            k_ref[:, b * HEAD : (b + 1) * HEAD] = both_ref[b, :, 0:HEAD].astype(jnp.float32)
            v_ref[:, b * HEAD : (b + 1) * HEAD] = both_ref[b, :, HEAD:].astype(jnp.float32)

    shape = jax.ShapeDtypeStruct((ROWS, MEMBERS * HEAD), jnp.float32)
    return pl.pallas_call(
        kernel,
        in_specs=[VMEM],
        out_specs=[VMEM, VMEM],
        out_shape=[shape, shape],
        name="kv_unpack",
    )(both)


def exchange(blocks):
    return lax.all_to_all(blocks, ("core", "head"), split_axis=0, concat_axis=0, tiled=True)


def shifted(block, by):
    count = lax.axis_size("group")
    pairs = [(i, i + by) for i in range(count) if 0 <= i + by < count]
    return lax.ppermute(block, "group", pairs)


def on_device(queries, keys, values, out_rows, output_gradient, log_norm_rows, doc_lengths):
    near = exchange(kv_pack(keys, values)).reshape(GROUP, 2 * HEAD)
    norms = log_norm_rows.T
    rows = []
    for chunk in range(CHUNKS):
        packed = rows_pack(queries, output_gradient, out_rows, norms, chunk)
        rows.append(exchange(packed))
    far1 = shifted(near, 1)
    relayed = relay(far1)
    far2 = shifted(relayed, 1)
    first_token = (lax.axis_index("group") * GROUP).astype(jnp.int32).reshape(1)
    results = []
    for chunk in range(CHUNKS):
        results = attention(doc_lengths, first_token, rows[chunk], far2, far1, near, results, chunk)
    q_all, far2_sum, far1_sum, near_sum = results
    back1 = shifted(far1_sum, -1)
    back2 = shifted(far2_sum, -2)
    q_back = exchange(q_all)
    both = exchange(kv_sum(near_sum, back1, back2))
    q_grad = q_unpack(q_back)
    key_gradient, value_gradient = kv_unpack(both)
    return (q_grad, key_gradient, value_gradient)


def solution(mesh):
    wide, head = mesh.shape["wide"], mesh.shape["head"]
    cores = MEMBERS // head
    finer = Mesh(mesh.devices.reshape(wide // cores, cores, head), ("group", "core", "head"))
    split = P(("group", "core", "head"), None)
    return jax.shard_map(
        on_device,
        mesh=finer,
        in_specs=(split,) * 6 + (P(),),
        out_specs=(split, split, split),
        check_vma=False,
    )
```

```python
import math

import jax
import jax.numpy as jnp
from jax import lax
from jax.experimental import pallas as pl
from jax.experimental.pallas import tpu as pltpu
from jax.sharding import Mesh, PartitionSpec as P


LOG2E = math.log2(math.e)
HEAD = 128
ROWS = 128
MEMBERS = 8
GROUP = MEMBERS * ROWS
FAR_BLOCKS = 14
FAR = FAR_BLOCKS * ROWS
FAR2 = FAR - GROUP
WINDOW = FAR + GROUP
HEADS = 8
CHUNKS = 2
H = HEADS // CHUNKS
WIDTH = H * HEAD
STATS = 2 * H
TQ = 256
TK = 256
NT = (((1,), (1,)), ((), ()))
TN = (((0,), (0,)), ((), ()))

SMEM = pl.BlockSpec(memory_space=pltpu.SMEM)
VMEM = pl.BlockSpec(memory_space=pltpu.VMEM)
ANY = pl.BlockSpec(memory_space=pl.ANY)
BIG = pltpu.CompilerParams(vmem_limit_bytes=56 << 20)


def kv_pack(keys, values):
    def kernel(k_ref, v_ref, out_ref):
        for b in range(MEMBERS):
            out_ref[b, :, 0:HEAD] = k_ref[:, b * HEAD : (b + 1) * HEAD]
            out_ref[b, :, HEAD : 2 * HEAD] = v_ref[:, b * HEAD : (b + 1) * HEAD]

    return pl.pallas_call(
        kernel,
        in_specs=[VMEM, VMEM],
        out_specs=VMEM,
        out_shape=jax.ShapeDtypeStruct((MEMBERS, ROWS, 2 * HEAD), jnp.bfloat16),
        name="kv_pack",
    )(keys, values)


def split_terms(value):
    high = value.astype(jnp.bfloat16)
    rest = value - high.astype(jnp.float32)
    middle = rest.astype(jnp.bfloat16)
    low = (rest - middle.astype(jnp.float32)).astype(jnp.bfloat16)
    return high, middle, low


def rows_pack(queries, grads, outs, norms, chunk):
    def kernel(q_ref, g_ref, o_ref, n_ref, out_ref, packed, forward, arrived, sent):
        def inbound(b):
            cut = pl.ds((b * CHUNKS + chunk) * WIDTH, WIDTH)
            return (
                pltpu.make_async_copy(
                    q_ref.at[:, cut], packed.at[b, pl.ds(0, ROWS), pl.ds(0, WIDTH)], arrived.at[0, b]
                ),
                pltpu.make_async_copy(
                    g_ref.at[:, cut],
                    packed.at[b, pl.ds(0, ROWS), pl.ds(WIDTH, WIDTH)],
                    arrived.at[1, b],
                ),
                pltpu.make_async_copy(o_ref.at[:, cut], forward.at[b], arrived.at[2, b]),
            )

        for b in range(MEMBERS):
            for copy in inbound(b):
                copy.start()
        lane = lax.broadcasted_iota(jnp.int32, (ROWS, 128), 1)
        for b in range(MEMBERS):
            for copy in inbound(b):
                copy.wait()
            deltas = jnp.zeros((ROWS, 128), jnp.float32)
            for h in range(H):
                cut = slice(h * HEAD, (h + 1) * HEAD)
                grad = packed[b, 0:ROWS, WIDTH + h * HEAD : WIDTH + (h + 1) * HEAD]
                product = grad.astype(jnp.float32) * forward[b, :, cut].astype(jnp.float32)
                deltas = jnp.where(lane == h, jnp.sum(product, axis=1, keepdims=True), deltas)
            first = b * HEADS + chunk * H
            stats = jnp.concatenate([n_ref[first : first + H], deltas.T[0:H]], axis=0)
            high, middle, low = split_terms(stats)
            packed[b, ROWS : ROWS + STATS, 0:ROWS] = high
            packed[b, ROWS : ROWS + STATS, ROWS : 2 * ROWS] = middle
            packed[b, ROWS : ROWS + STATS, 2 * ROWS : 3 * ROWS] = low
            packed[b, ROWS : ROWS + STATS, 3 * ROWS :] = jnp.zeros(
                (STATS, 2 * WIDTH - 3 * ROWS), jnp.bfloat16
            )
            pltpu.make_async_copy(packed.at[b], out_ref.at[b], sent.at[b]).start()
        for b in range(MEMBERS):
            pltpu.make_async_copy(packed.at[b], out_ref.at[b], sent.at[b]).wait()

    shape = (MEMBERS, ROWS + STATS, 2 * WIDTH)
    return pl.pallas_call(
        kernel,
        in_specs=[ANY, ANY, ANY, VMEM],
        out_specs=ANY,
        out_shape=jax.ShapeDtypeStruct(shape, jnp.bfloat16),
        scratch_shapes=[
            pltpu.VMEM(shape, jnp.bfloat16),
            pltpu.VMEM((MEMBERS, ROWS, WIDTH), jnp.bfloat16),
            pltpu.SemaphoreType.DMA((3, MEMBERS)),
            pltpu.SemaphoreType.DMA((MEMBERS,)),
        ],
        compiler_params=BIG,
        name="rows_pack",
    )(queries, grads, outs, norms)


def relay(block):
    def kernel(block_ref, out_ref):
        out_ref[...] = block_ref[GROUP - FAR2 :]

    return pl.pallas_call(
        kernel,
        in_specs=[VMEM],
        out_specs=VMEM,
        out_shape=jax.ShapeDtypeStruct((FAR2, 2 * HEAD), jnp.bfloat16),
        name="relay",
    )(block)


def attention(doc_lengths, first_token, rows, far2, far1, near, earlier, chunk):
    scaling = 1.0 / math.sqrt(HEAD)
    docs = doc_lengths.shape[0]
    parts = TQ // ROWS
    last = chunk == CHUNKS - 1

    def kernel(lengths_ref, first_ref, rows_ref, far2_ref, far1_ref, near_ref, *rest):
        if last:
            sums_ref, q_out, far2_out, far1_out, near_out, window, acc, q_acc = rest
        else:
            q_out, acc, window, q_acc = rest
        window[0:FAR2] = far2_ref[...]
        window[FAR2:FAR] = far1_ref[...]
        window[FAR:WINDOW] = near_ref[...]
        if last:
            acc[...] = sums_ref[...]
        else:
            acc[...] = jnp.zeros_like(acc)
        group_first = first_ref[0]
        window_first = group_first - FAR

        def query_tile(tile, carry):
            token = group_first + tile * TQ
            position = token + lax.broadcasted_iota(jnp.int32, (8, TQ), 1)
            start = jnp.int32(0)
            doc_first = start
            doc_start = jnp.zeros((8, TQ), jnp.int32)
            for doc in range(1, docs):
                start = start + lengths_ref[doc - 1]
                doc_first = jnp.where(start <= token, start, doc_first)
                doc_start = jnp.where(start <= position, start, doc_start)
            low = doc_start[0:1] - window_first
            reach = position[0:1] - doc_start[0:1]
            key_begin = (doc_first - window_first) // TK
            key_end = (token + TQ - 1 - window_first) // TK + 1
            block = tile * parts
            pairs = [(h, s) for h in range(H) for s in range(parts)]
            query = jnp.concatenate(
                [rows_ref[block + s, 0:ROWS, h * HEAD : (h + 1) * HEAD] for h, s in pairs], axis=0
            )
            grad = jnp.concatenate(
                [rows_ref[block + s, 0:ROWS, WIDTH + h * HEAD : WIDTH + (h + 1) * HEAD] for h, s in pairs],
                axis=0,
            )
            stats = [
                sum(
                    rows_ref[block + s, ROWS : ROWS + STATS, t * ROWS : (t + 1) * ROWS].astype(
                        jnp.float32
                    )
                    for t in (2, 1, 0)
                )
                for s in range(parts)
            ]
            norm = LOG2E * jnp.concatenate([stats[s][h : h + 1] for h, s in pairs], axis=1)
            delta = jnp.concatenate([stats[s][H + h : H + h + 1] for h, s in pairs], axis=1)
            q_acc[...] = jnp.zeros_like(q_acc)

            def key_tile(index, inner):
                row = pl.multiple_of(index * TK, TK)
                k_rows = window[pl.ds(row, TK), 0:HEAD]
                v_rows = window[pl.ds(row, TK), HEAD : 2 * HEAD]
                offset = row + lax.broadcasted_iota(jnp.int32, (TK, TQ), 0) - low
                allowed = (offset >= 0) & (offset <= reach)
                allowed = jnp.concatenate([allowed] * H, axis=1)
                scores = lax.dot_general(k_rows, query, NT, preferred_element_type=jnp.float32)
                attend = jnp.where(allowed, jnp.exp2(scores * (scaling * LOG2E) - norm), 0.0)
                prob_grad = lax.dot_general(v_rows, grad, NT, preferred_element_type=jnp.float32)
                score_low = (attend * (prob_grad - delta)).astype(jnp.bfloat16)
                attend_low = attend.astype(jnp.bfloat16)
                acc[pl.ds(row, TK), HEAD : 2 * HEAD] += jnp.dot(
                    attend_low, grad, preferred_element_type=jnp.float32
                )
                acc[pl.ds(row, TK), 0:HEAD] += jnp.dot(
                    score_low, query, preferred_element_type=jnp.float32
                )
                q_acc[...] += lax.dot_general(
                    score_low, k_rows, TN, preferred_element_type=jnp.float32
                )
                return inner

            lax.fori_loop(key_begin, key_end, key_tile, 0)
            for at_row, (h, s) in enumerate(pairs):
                part = q_acc[at_row * ROWS : (at_row + 1) * ROWS, :] * scaling
                q_out[block + s, :, h * HEAD : (h + 1) * HEAD] = part.astype(jnp.bfloat16)
            return carry

        lax.fori_loop(0, GROUP // TQ, query_tile, 0)
        if last:
            for ref, begin, end in (
                (far2_out, 0, FAR2),
                (far1_out, FAR2, FAR),
                (near_out, FAR, WINDOW),
            ):
                ref[:, 0:HEAD] = (acc[begin:end, 0:HEAD] * scaling).astype(ref.dtype)
                ref[:, HEAD : 2 * HEAD] = acc[begin:end, HEAD : 2 * HEAD].astype(ref.dtype)

    pair = 2 * HEAD
    q_shape = jax.ShapeDtypeStruct((MEMBERS, ROWS, WIDTH), jnp.bfloat16)
    acc_shape = (WINDOW, pair)
    window_scratch = pltpu.VMEM((WINDOW, pair), jnp.bfloat16)
    q_scratch = pltpu.VMEM((H * TQ, HEAD), jnp.float32)
    if last:
        out_shape = [
            q_shape,
            jax.ShapeDtypeStruct((FAR2, pair), jnp.bfloat16),
            jax.ShapeDtypeStruct((GROUP, pair), jnp.bfloat16),
            jax.ShapeDtypeStruct((GROUP, pair), jnp.float32),
        ]
        scratch = [window_scratch, pltpu.VMEM(acc_shape, jnp.float32), q_scratch]
    else:
        out_shape = [q_shape, jax.ShapeDtypeStruct(acc_shape, jnp.float32)]
        scratch = [window_scratch, q_scratch]
    operands = [doc_lengths, first_token, rows, far2, far1, near, *earlier]
    return pl.pallas_call(
        kernel,
        in_specs=[SMEM, SMEM] + [VMEM] * (len(operands) - 2),
        out_specs=[VMEM] * len(out_shape),
        out_shape=out_shape,
        scratch_shapes=scratch,
        compiler_params=BIG,
    )(*operands)


def kv_sum(near, back1, back2):
    def kernel(near_ref, back1_ref, back2_ref, out_ref):
        for b in range(MEMBERS):
            cut = slice(b * ROWS, (b + 1) * ROWS)
            total = near_ref[cut] + back1_ref[cut].astype(jnp.float32)
            skip = (GROUP - FAR2) // ROWS
            if b >= skip:
                far = slice((b - skip) * ROWS, (b - skip + 1) * ROWS)
                total = total + back2_ref[far].astype(jnp.float32)
            out_ref[b] = total.astype(jnp.bfloat16)

    return pl.pallas_call(
        kernel,
        in_specs=[VMEM] * 3,
        out_specs=VMEM,
        out_shape=jax.ShapeDtypeStruct((MEMBERS, ROWS, 2 * HEAD), jnp.bfloat16),
        name="kv_sum",
    )(near, back1, back2)


def q_unpack(parts):
    def kernel(*refs):
        sources, (out_ref, narrow, wide, arrived, sent) = refs[:CHUNKS], refs[CHUNKS:]
        pieces = [(chunk, b) for chunk in range(CHUNKS) for b in range(MEMBERS)]

        def inbound(chunk, b):
            return pltpu.make_async_copy(
                sources[chunk].at[b], narrow.at[chunk, b], arrived.at[chunk, b]
            )

        def outbound(chunk, b):
            cut = pl.ds((b * CHUNKS + chunk) * WIDTH, WIDTH)
            return pltpu.make_async_copy(
                wide.at[chunk, b], out_ref.at[:, cut], sent.at[chunk, b]
            )

        for piece in pieces:
            inbound(*piece).start()
        for chunk, b in pieces:
            inbound(chunk, b).wait()
            wide[chunk, b] = narrow[chunk, b].astype(jnp.float32)
            outbound(chunk, b).start()
        for piece in pieces:
            outbound(*piece).wait()

    shape = (CHUNKS, MEMBERS, ROWS, WIDTH)
    return pl.pallas_call(
        kernel,
        in_specs=[ANY] * CHUNKS,
        out_specs=ANY,
        out_shape=jax.ShapeDtypeStruct((ROWS, MEMBERS * CHUNKS * WIDTH), jnp.float32),
        scratch_shapes=[
            pltpu.VMEM(shape, jnp.bfloat16),
            pltpu.VMEM(shape, jnp.float32),
            pltpu.SemaphoreType.DMA((CHUNKS, MEMBERS)),
            pltpu.SemaphoreType.DMA((CHUNKS, MEMBERS)),
        ],
        compiler_params=BIG,
        name="q_unpack",
    )(*parts)


def kv_unpack(both):
    def kernel(both_ref, k_ref, v_ref):
        for b in range(MEMBERS):
            k_ref[:, b * HEAD : (b + 1) * HEAD] = both_ref[b, :, 0:HEAD].astype(jnp.float32)
            v_ref[:, b * HEAD : (b + 1) * HEAD] = both_ref[b, :, HEAD:].astype(jnp.float32)

    shape = jax.ShapeDtypeStruct((ROWS, MEMBERS * HEAD), jnp.float32)
    return pl.pallas_call(
        kernel,
        in_specs=[VMEM],
        out_specs=[VMEM, VMEM],
        out_shape=[shape, shape],
        name="kv_unpack",
    )(both)


def exchange(blocks):
    return lax.all_to_all(blocks, ("core", "head"), split_axis=0, concat_axis=0, tiled=True)


def shifted(block, by):
    count = lax.axis_size("group")
    pairs = [(i, i + by) for i in range(count) if 0 <= i + by < count]
    return lax.ppermute(block, "group", pairs)


def on_device(queries, keys, values, out_rows, output_gradient, log_norm_rows, doc_lengths):
    near = exchange(kv_pack(keys, values)).reshape(GROUP, 2 * HEAD)
    norms = log_norm_rows.T
    rows = []
    for chunk in range(CHUNKS):
        packed = rows_pack(queries, output_gradient, out_rows, norms, chunk)
        rows.append(exchange(packed))
    far1 = shifted(near, 1)
    relayed = relay(far1)
    far2 = shifted(relayed, 1)
    first_token = (lax.axis_index("group") * GROUP).astype(jnp.int32).reshape(1)
    sums, q_back = [], []
    for chunk in range(CHUNKS):
        q_part, *sums = attention(
            doc_lengths, first_token, rows[chunk], far2, far1, near, sums, chunk
        )
        q_back.append(exchange(q_part))
    far2_sum, far1_sum, near_sum = sums
    back1 = shifted(far1_sum, -1)
    back2 = shifted(far2_sum, -2)
    both = exchange(kv_sum(near_sum, back1, back2))
    q_grad = q_unpack(q_back)
    key_gradient, value_gradient = kv_unpack(both)
    return (q_grad, key_gradient, value_gradient)


def solution(mesh):
    wide, head = mesh.shape["wide"], mesh.shape["head"]
    cores = MEMBERS // head
    finer = Mesh(mesh.devices.reshape(wide // cores, cores, head), ("group", "core", "head"))
    split = P(("group", "core", "head"), None)
    return jax.shard_map(
        on_device,
        mesh=finer,
        in_specs=(split,) * 6 + (P(),),
        out_specs=(split, split, split),
        check_vma=False,
    )
```

```python
import math

import jax
import jax.numpy as jnp
from jax import lax
from jax.experimental import pallas as pl
from jax.experimental.pallas import tpu as pltpu
from jax.sharding import Mesh, PartitionSpec as P


LOG2E = math.log2(math.e)
MASKED = -1e30
HEAD = 128
ROWS = 128
MEMBERS = 8
GROUP = MEMBERS * ROWS
FAR_BLOCKS = 14
FAR = FAR_BLOCKS * ROWS
FAR2 = FAR - GROUP
WINDOW = FAR + GROUP
HEADS = 8
CHUNKS = 2
H = HEADS // CHUNKS
WIDTH = H * HEAD
STATS = 2 * H
TQ = 256
TK = 256
NT = (((1,), (1,)), ((), ()))
TN = (((0,), (0,)), ((), ()))

SMEM = pl.BlockSpec(memory_space=pltpu.SMEM)
VMEM = pl.BlockSpec(memory_space=pltpu.VMEM)
ANY = pl.BlockSpec(memory_space=pl.ANY)
BIG = pltpu.CompilerParams(vmem_limit_bytes=56 << 20)


def kv_pack(keys, values):
    def kernel(k_ref, v_ref, out_ref):
        for b in range(MEMBERS):
            out_ref[b, :, 0:HEAD] = k_ref[:, b * HEAD : (b + 1) * HEAD]
            out_ref[b, :, HEAD : 2 * HEAD] = v_ref[:, b * HEAD : (b + 1) * HEAD]

    return pl.pallas_call(
        kernel,
        in_specs=[VMEM, VMEM],
        out_specs=VMEM,
        out_shape=jax.ShapeDtypeStruct((MEMBERS, ROWS, 2 * HEAD), jnp.bfloat16),
        name="kv_pack",
    )(keys, values)


def split_terms(value):
    high = value.astype(jnp.bfloat16)
    rest = value - high.astype(jnp.float32)
    middle = rest.astype(jnp.bfloat16)
    low = (rest - middle.astype(jnp.float32)).astype(jnp.bfloat16)
    return high, middle, low


def rows_pack(queries, grads, outs, norms, chunk):
    def kernel(q_ref, g_ref, o_ref, n_ref, out_ref, packed, forward, arrived, sent):
        def inbound(b):
            cut = pl.ds((b * CHUNKS + chunk) * WIDTH, WIDTH)
            return (
                pltpu.make_async_copy(
                    q_ref.at[:, cut], packed.at[b, pl.ds(0, ROWS), pl.ds(0, WIDTH)], arrived.at[0, b]
                ),
                pltpu.make_async_copy(
                    g_ref.at[:, cut],
                    packed.at[b, pl.ds(0, ROWS), pl.ds(WIDTH, WIDTH)],
                    arrived.at[1, b],
                ),
                pltpu.make_async_copy(o_ref.at[:, cut], forward.at[b], arrived.at[2, b]),
            )

        for b in range(MEMBERS):
            for copy in inbound(b):
                copy.start()
        lane = lax.broadcasted_iota(jnp.int32, (ROWS, 128), 1)
        for b in range(MEMBERS):
            for copy in inbound(b):
                copy.wait()
            deltas = jnp.zeros((ROWS, 128), jnp.float32)
            for h in range(H):
                cut = slice(h * HEAD, (h + 1) * HEAD)
                grad = packed[b, 0:ROWS, WIDTH + h * HEAD : WIDTH + (h + 1) * HEAD]
                product = grad.astype(jnp.float32) * forward[b, :, cut].astype(jnp.float32)
                deltas = jnp.where(lane == h, jnp.sum(product, axis=1, keepdims=True), deltas)
            first = b * HEADS + chunk * H
            stats = jnp.concatenate([n_ref[first : first + H], deltas.T[0:H]], axis=0)
            high, middle, low = split_terms(stats)
            packed[b, ROWS : ROWS + STATS, 0:ROWS] = high
            packed[b, ROWS : ROWS + STATS, ROWS : 2 * ROWS] = middle
            packed[b, ROWS : ROWS + STATS, 2 * ROWS : 3 * ROWS] = low
            packed[b, ROWS : ROWS + STATS, 3 * ROWS :] = jnp.zeros(
                (STATS, 2 * WIDTH - 3 * ROWS), jnp.bfloat16
            )
            pltpu.make_async_copy(packed.at[b], out_ref.at[b], sent.at[b]).start()
        for b in range(MEMBERS):
            pltpu.make_async_copy(packed.at[b], out_ref.at[b], sent.at[b]).wait()

    shape = (MEMBERS, ROWS + STATS, 2 * WIDTH)
    return pl.pallas_call(
        kernel,
        in_specs=[ANY, ANY, ANY, VMEM],
        out_specs=ANY,
        out_shape=jax.ShapeDtypeStruct(shape, jnp.bfloat16),
        scratch_shapes=[
            pltpu.VMEM(shape, jnp.bfloat16),
            pltpu.VMEM((MEMBERS, ROWS, WIDTH), jnp.bfloat16),
            pltpu.SemaphoreType.DMA((3, MEMBERS)),
            pltpu.SemaphoreType.DMA((MEMBERS,)),
        ],
        compiler_params=BIG,
        name="rows_pack",
    )(queries, grads, outs, norms)


def relay(block):
    def kernel(block_ref, out_ref):
        out_ref[...] = block_ref[GROUP - FAR2 :]

    return pl.pallas_call(
        kernel,
        in_specs=[VMEM],
        out_specs=VMEM,
        out_shape=jax.ShapeDtypeStruct((FAR2, 2 * HEAD), jnp.bfloat16),
        name="relay",
    )(block)


def attention(doc_lengths, first_token, rows, far2, far1, near, earlier, chunk):
    scaling = 1.0 / math.sqrt(HEAD)
    docs = doc_lengths.shape[0]
    parts = TQ // ROWS
    last = chunk == CHUNKS - 1

    def kernel(lengths_ref, first_ref, rows_hbm, far2_ref, far1_ref, near_ref, *rest):
        if last:
            sums_ref, q_hbm, far2_out, far1_out, near_out, *scratch = rest
            rows_ref, q_ref, window, acc, q_acc, row_sem, key_sem, q_sem, sums, sums_sem = scratch
            sums_copy = pltpu.make_async_copy(sums_ref, sums, sums_sem)
        else:
            q_hbm, sums_out, *scratch = rest
            rows_ref, q_ref, window, acc, q_acc, row_sem, key_sem, q_sem = scratch

        def rows_copy(tile):
            cut = pl.ds(tile * parts, parts)
            return pltpu.make_async_copy(rows_hbm.at[cut], rows_ref.at[cut], row_sem.at[tile])

        def q_copy(tile):
            cut = pl.ds(tile * parts, parts)
            return pltpu.make_async_copy(q_ref.at[cut], q_hbm.at[cut], q_sem.at[tile])

        key_copies = [
            pltpu.make_async_copy(ref, window.at[pl.ds(begin, size)], key_sem.at[i])
            for i, (ref, begin, size) in enumerate(
                ((far2_ref, 0, FAR2), (far1_ref, FAR2, GROUP), (near_ref, FAR, GROUP))
            )
        ]
        for copy in key_copies:
            copy.start()
        for tile in range(GROUP // TQ):
            rows_copy(tile).start()
        if last:
            sums_copy.start()
        acc[...] = jnp.zeros_like(acc)
        for copy in key_copies:
            copy.wait()
        group_first = first_ref[0]
        window_first = group_first - FAR

        def query_tile(tile, carry):
            token = group_first + tile * TQ
            position = token + lax.broadcasted_iota(jnp.int32, (8, TQ), 1)
            start = jnp.int32(0)
            doc_first = start
            doc_start = jnp.zeros((8, TQ), jnp.int32)
            for doc in range(1, docs):
                start = start + lengths_ref[doc - 1]
                doc_first = jnp.where(start <= token, start, doc_first)
                doc_start = jnp.where(start <= position, start, doc_start)
            low = doc_start[0:1] - window_first
            reach = position[0:1] - doc_start[0:1]
            key_begin = (doc_first - window_first) // TK
            key_end = (token + TQ - 1 - window_first) // TK + 1
            block = tile * parts
            rows_copy(tile).wait()
            pairs = [(h, s) for h in range(H) for s in range(parts)]
            query = jnp.concatenate(
                [rows_ref[block + s, 0:ROWS, h * HEAD : (h + 1) * HEAD] for h, s in pairs], axis=0
            )
            grad = jnp.concatenate(
                [rows_ref[block + s, 0:ROWS, WIDTH + h * HEAD : WIDTH + (h + 1) * HEAD] for h, s in pairs],
                axis=0,
            )
            stats = [
                sum(
                    rows_ref[block + s, ROWS : ROWS + STATS, t * ROWS : (t + 1) * ROWS].astype(
                        jnp.float32
                    )
                    for t in (2, 1, 0)
                )
                for s in range(parts)
            ]
            norm = LOG2E * jnp.concatenate([stats[s][h : h + 1] for h, s in pairs], axis=1)
            delta = jnp.concatenate([stats[s][H + h : H + h + 1] for h, s in pairs], axis=1)
            q_acc[...] = jnp.zeros_like(q_acc)

            def key_tile(index, inner):
                row = pl.multiple_of(index * TK, TK)
                k_rows = window[pl.ds(row, TK), 0:HEAD]
                v_rows = window[pl.ds(row, TK), HEAD : 2 * HEAD]
                offset = row + lax.broadcasted_iota(jnp.int32, (TK, TQ), 0) - low
                allowed = (offset >= 0) & (offset <= reach)
                bias = jnp.concatenate([jnp.where(allowed, 0.0, MASKED)] * H, axis=1)
                scores = lax.dot_general(k_rows, query, NT, preferred_element_type=jnp.float32)
                attend = jnp.exp2(scores * (scaling * LOG2E) - norm + bias)
                prob_grad = lax.dot_general(v_rows, grad, NT, preferred_element_type=jnp.float32)
                score_low = (attend * (prob_grad - delta)).astype(jnp.bfloat16)
                attend_low = attend.astype(jnp.bfloat16)
                acc[pl.ds(row, TK), HEAD : 2 * HEAD] += jnp.dot(
                    attend_low, grad, preferred_element_type=jnp.float32
                )
                acc[pl.ds(row, TK), 0:HEAD] += jnp.dot(
                    score_low, query, preferred_element_type=jnp.float32
                )
                q_acc[...] += lax.dot_general(
                    score_low, k_rows, TN, preferred_element_type=jnp.float32
                )
                return inner

            lax.fori_loop(key_begin, key_end, key_tile, 0)
            for at_row, (h, s) in enumerate(pairs):
                part = q_acc[at_row * ROWS : (at_row + 1) * ROWS, :] * scaling
                q_ref[block + s, :, h * HEAD : (h + 1) * HEAD] = part.astype(jnp.bfloat16)
            q_copy(tile).start()
            return carry

        lax.fori_loop(0, GROUP // TQ, query_tile, 0)
        if last:
            sums_copy.wait()
            for ref, begin, end in (
                (far2_out, 0, FAR2),
                (far1_out, FAR2, FAR),
                (near_out, FAR, WINDOW),
            ):
                total = acc[begin:end] + sums[begin:end]
                ref[:, 0:HEAD] = (total[:, 0:HEAD] * scaling).astype(ref.dtype)
                ref[:, HEAD : 2 * HEAD] = total[:, HEAD : 2 * HEAD].astype(ref.dtype)
        else:
            pltpu.sync_copy(acc, sums_out)
        for tile in range(GROUP // TQ):
            q_copy(tile).wait()

    pair = 2 * HEAD
    q_shape = jax.ShapeDtypeStruct((MEMBERS, ROWS, WIDTH), jnp.bfloat16)
    acc_shape = (WINDOW, pair)
    tiles = GROUP // TQ
    scratch = [
        pltpu.VMEM((MEMBERS, ROWS + STATS, 2 * WIDTH), jnp.bfloat16),
        pltpu.VMEM(q_shape.shape, q_shape.dtype),
        pltpu.VMEM((WINDOW, pair), jnp.bfloat16),
        pltpu.VMEM(acc_shape, jnp.float32),
        pltpu.VMEM((H * TQ, HEAD), jnp.float32),
        pltpu.SemaphoreType.DMA((tiles,)),
        pltpu.SemaphoreType.DMA((3,)),
        pltpu.SemaphoreType.DMA((tiles,)),
    ]
    if last:
        out_shape = [
            q_shape,
            jax.ShapeDtypeStruct((FAR2, pair), jnp.bfloat16),
            jax.ShapeDtypeStruct((GROUP, pair), jnp.bfloat16),
            jax.ShapeDtypeStruct((GROUP, pair), jnp.float32),
        ]
        out_specs = [ANY, VMEM, VMEM, VMEM]
        scratch += [pltpu.VMEM(acc_shape, jnp.float32), pltpu.SemaphoreType.DMA]
    else:
        out_shape = [q_shape, jax.ShapeDtypeStruct(acc_shape, jnp.float32)]
        out_specs = [ANY, ANY]
    operands = [doc_lengths, first_token, rows, far2, far1, near, *earlier]
    return pl.pallas_call(
        kernel,
        in_specs=[SMEM, SMEM] + [ANY] * (len(operands) - 2),
        out_specs=out_specs,
        out_shape=out_shape,
        scratch_shapes=scratch,
        compiler_params=BIG,
    )(*operands)


def kv_sum(near, back1, back2):
    skip = (GROUP - FAR2) // ROWS

    def kernel(near_hbm, back1_hbm, back2_hbm, out_hbm, near_ref, back1_ref, back2_ref, out_ref, sems):
        def inbound(b):
            cut = pl.ds(b * ROWS, ROWS)
            copies = [
                pltpu.make_async_copy(near_hbm.at[cut], near_ref.at[cut], sems.at[0, b]),
                pltpu.make_async_copy(back1_hbm.at[cut], back1_ref.at[cut], sems.at[1, b]),
            ]
            if b >= skip:
                far = pl.ds((b - skip) * ROWS, ROWS)
                copies.append(
                    pltpu.make_async_copy(back2_hbm.at[far], back2_ref.at[far], sems.at[2, b])
                )
            return copies

        def outbound(b):
            return pltpu.make_async_copy(out_ref.at[b], out_hbm.at[b], sems.at[3, b])

        for b in range(MEMBERS):
            for copy in inbound(b):
                copy.start()
        for b in range(MEMBERS):
            for copy in inbound(b):
                copy.wait()
            cut = slice(b * ROWS, (b + 1) * ROWS)
            total = near_ref[cut] + back1_ref[cut].astype(jnp.float32)
            if b >= skip:
                far = slice((b - skip) * ROWS, (b - skip + 1) * ROWS)
                total = total + back2_ref[far].astype(jnp.float32)
            out_ref[b] = total.astype(jnp.bfloat16)
            outbound(b).start()
        for b in range(MEMBERS):
            outbound(b).wait()

    shape = (MEMBERS, ROWS, 2 * HEAD)
    return pl.pallas_call(
        kernel,
        in_specs=[ANY] * 3,
        out_specs=ANY,
        out_shape=jax.ShapeDtypeStruct(shape, jnp.bfloat16),
        scratch_shapes=[pltpu.VMEM(a.shape, a.dtype) for a in (near, back1, back2)]
        + [pltpu.VMEM(shape, jnp.bfloat16), pltpu.SemaphoreType.DMA((4, MEMBERS))],
        compiler_params=BIG,
        name="kv_sum",
    )(near, back1, back2)


def q_unpack(parts):
    def kernel(*refs):
        sources, (out_ref, narrow, wide, arrived, sent) = refs[:CHUNKS], refs[CHUNKS:]
        pieces = [(chunk, b) for chunk in range(CHUNKS) for b in range(MEMBERS)]

        def inbound(chunk, b):
            return pltpu.make_async_copy(
                sources[chunk].at[b], narrow.at[chunk, b], arrived.at[chunk, b]
            )

        def outbound(chunk, b):
            cut = pl.ds((b * CHUNKS + chunk) * WIDTH, WIDTH)
            return pltpu.make_async_copy(
                wide.at[chunk, b], out_ref.at[:, cut], sent.at[chunk, b]
            )

        for piece in pieces:
            inbound(*piece).start()
        for chunk, b in pieces:
            inbound(chunk, b).wait()
            wide[chunk, b] = narrow[chunk, b].astype(jnp.float32)
            outbound(chunk, b).start()
        for piece in pieces:
            outbound(*piece).wait()

    shape = (CHUNKS, MEMBERS, ROWS, WIDTH)
    return pl.pallas_call(
        kernel,
        in_specs=[ANY] * CHUNKS,
        out_specs=ANY,
        out_shape=jax.ShapeDtypeStruct((ROWS, MEMBERS * CHUNKS * WIDTH), jnp.float32),
        scratch_shapes=[
            pltpu.VMEM(shape, jnp.bfloat16),
            pltpu.VMEM(shape, jnp.float32),
            pltpu.SemaphoreType.DMA((CHUNKS, MEMBERS)),
            pltpu.SemaphoreType.DMA((CHUNKS, MEMBERS)),
        ],
        compiler_params=BIG,
        name="q_unpack",
    )(*parts)


def kv_unpack(both):
    def kernel(both_hbm, k_hbm, v_hbm, both_ref, k_ref, v_ref, sems):
        def inbound(b):
            return pltpu.make_async_copy(both_hbm.at[b], both_ref.at[b], sems.at[0, b])

        def outbound(b):
            cut = pl.ds(b * HEAD, HEAD)
            return (
                pltpu.make_async_copy(k_ref.at[b], k_hbm.at[:, cut], sems.at[1, b]),
                pltpu.make_async_copy(v_ref.at[b], v_hbm.at[:, cut], sems.at[2, b]),
            )

        for b in range(MEMBERS):
            inbound(b).start()
        for b in range(MEMBERS):
            inbound(b).wait()
            k_ref[b] = both_ref[b, :, 0:HEAD].astype(jnp.float32)
            v_ref[b] = both_ref[b, :, HEAD:].astype(jnp.float32)
            for copy in outbound(b):
                copy.start()
        for b in range(MEMBERS):
            for copy in outbound(b):
                copy.wait()

    shape = jax.ShapeDtypeStruct((ROWS, MEMBERS * HEAD), jnp.float32)
    halves = pltpu.VMEM((MEMBERS, ROWS, HEAD), jnp.float32)
    return pl.pallas_call(
        kernel,
        in_specs=[ANY],
        out_specs=[ANY, ANY],
        out_shape=[shape, shape],
        scratch_shapes=[
            pltpu.VMEM((MEMBERS, ROWS, 2 * HEAD), jnp.bfloat16),
            halves,
            halves,
            pltpu.SemaphoreType.DMA((3, MEMBERS)),
        ],
        compiler_params=BIG,
        name="kv_unpack",
    )(both)


def exchange(blocks):
    return lax.all_to_all(blocks, ("core", "head"), split_axis=0, concat_axis=0, tiled=True)


def shifted(block, by):
    count = lax.axis_size("group")
    pairs = [(i, i + by) for i in range(count) if 0 <= i + by < count]
    return lax.ppermute(block, "group", pairs)


def on_device(queries, keys, values, out_rows, output_gradient, log_norm_rows, doc_lengths):
    near = exchange(kv_pack(keys, values)).reshape(GROUP, 2 * HEAD)
    norms = log_norm_rows.T
    rows = []
    for chunk in range(CHUNKS):
        packed = rows_pack(queries, output_gradient, out_rows, norms, chunk)
        rows.append(exchange(packed))
    far1 = shifted(near, 1)
    relayed = relay(far1)
    far2 = shifted(relayed, 1)
    first_token = (lax.axis_index("group") * GROUP).astype(jnp.int32).reshape(1)
    sums, q_back = [], []
    for chunk in range(CHUNKS):
        q_part, *sums = attention(
            doc_lengths, first_token, rows[chunk], far2, far1, near, sums, chunk
        )
        q_back.append(exchange(q_part))
    far2_sum, far1_sum, near_sum = sums
    back1 = shifted(far1_sum, -1)
    back2 = shifted(far2_sum, -2)
    both = exchange(kv_sum(near_sum, back1, back2))
    q_grad = q_unpack(q_back)
    key_gradient, value_gradient = kv_unpack(both)
    return (q_grad, key_gradient, value_gradient)


def solution(mesh):
    wide, head = mesh.shape["wide"], mesh.shape["head"]
    cores = MEMBERS // head
    finer = Mesh(mesh.devices.reshape(wide // cores, cores, head), ("group", "core", "head"))
    split = P(("group", "core", "head"), None)
    return jax.shard_map(
        on_device,
        mesh=finer,
        in_specs=(split,) * 6 + (P(),),
        out_specs=(split, split, split),
        check_vma=False,
    )
```

```python
import math

import jax
import jax.numpy as jnp
from jax import lax
from jax.experimental import pallas as pl
from jax.experimental.pallas import tpu as pltpu
from jax.sharding import Mesh, PartitionSpec as P


LOG2E = math.log2(math.e)
MASKED = -1e30
HEAD = 128
ROWS = 128
MEMBERS = 8
GROUP = MEMBERS * ROWS
FAR_BLOCKS = 14
FAR = FAR_BLOCKS * ROWS
FAR2 = FAR - GROUP
WINDOW = FAR + GROUP
HEADS = 8
CHUNKS = 2
H = HEADS // CHUNKS
WIDTH = H * HEAD
STATS = 2 * H
TQ = 256
TK = 256
NT = (((1,), (1,)), ((), ()))
TN = (((0,), (0,)), ((), ()))

SMEM = pl.BlockSpec(memory_space=pltpu.SMEM)
VMEM = pl.BlockSpec(memory_space=pltpu.VMEM)
ANY = pl.BlockSpec(memory_space=pl.ANY)
BIG = pltpu.CompilerParams(vmem_limit_bytes=56 << 20)


def kv_pack(keys, values):
    def kernel(k_ref, v_ref, out_ref):
        for b in range(MEMBERS):
            out_ref[b, :, 0:HEAD] = k_ref[:, b * HEAD : (b + 1) * HEAD]
            out_ref[b, :, HEAD : 2 * HEAD] = v_ref[:, b * HEAD : (b + 1) * HEAD]

    return pl.pallas_call(
        kernel,
        in_specs=[VMEM, VMEM],
        out_specs=VMEM,
        out_shape=jax.ShapeDtypeStruct((MEMBERS, ROWS, 2 * HEAD), jnp.bfloat16),
        name="kv_pack",
    )(keys, values)


def split_terms(value):
    high = value.astype(jnp.bfloat16)
    rest = value - high.astype(jnp.float32)
    middle = rest.astype(jnp.bfloat16)
    low = (rest - middle.astype(jnp.float32)).astype(jnp.bfloat16)
    return high, middle, low


def rows_pack(queries, grads, outs, norms, chunk):
    def kernel(q_ref, g_ref, o_ref, n_ref, out_ref, packed, forward, arrived, sent):
        def inbound(b):
            cut = pl.ds((b * CHUNKS + chunk) * WIDTH, WIDTH)
            return (
                pltpu.make_async_copy(
                    q_ref.at[:, cut], packed.at[b, pl.ds(0, ROWS), pl.ds(0, WIDTH)], arrived.at[0, b]
                ),
                pltpu.make_async_copy(
                    g_ref.at[:, cut],
                    packed.at[b, pl.ds(0, ROWS), pl.ds(WIDTH, WIDTH)],
                    arrived.at[1, b],
                ),
                pltpu.make_async_copy(o_ref.at[:, cut], forward.at[b], arrived.at[2, b]),
            )

        for b in range(MEMBERS):
            for copy in inbound(b):
                copy.start()
        lane = lax.broadcasted_iota(jnp.int32, (ROWS, 128), 1)
        for b in range(MEMBERS):
            for copy in inbound(b):
                copy.wait()
            deltas = jnp.zeros((ROWS, 128), jnp.float32)
            for h in range(H):
                cut = slice(h * HEAD, (h + 1) * HEAD)
                grad = packed[b, 0:ROWS, WIDTH + h * HEAD : WIDTH + (h + 1) * HEAD]
                product = grad.astype(jnp.float32) * forward[b, :, cut].astype(jnp.float32)
                deltas = jnp.where(lane == h, jnp.sum(product, axis=1, keepdims=True), deltas)
            first = b * HEADS + chunk * H
            stats = jnp.concatenate([n_ref[first : first + H], deltas.T[0:H]], axis=0)
            high, middle, low = split_terms(stats)
            packed[b, ROWS : ROWS + STATS, 0:ROWS] = high
            packed[b, ROWS : ROWS + STATS, ROWS : 2 * ROWS] = middle
            packed[b, ROWS : ROWS + STATS, 2 * ROWS : 3 * ROWS] = low
            packed[b, ROWS : ROWS + STATS, 3 * ROWS :] = jnp.zeros(
                (STATS, 2 * WIDTH - 3 * ROWS), jnp.bfloat16
            )
            pltpu.make_async_copy(packed.at[b], out_ref.at[b], sent.at[b]).start()
        for b in range(MEMBERS):
            pltpu.make_async_copy(packed.at[b], out_ref.at[b], sent.at[b]).wait()

    shape = (MEMBERS, ROWS + STATS, 2 * WIDTH)
    return pl.pallas_call(
        kernel,
        in_specs=[ANY, ANY, ANY, VMEM],
        out_specs=ANY,
        out_shape=jax.ShapeDtypeStruct(shape, jnp.bfloat16),
        scratch_shapes=[
            pltpu.VMEM(shape, jnp.bfloat16),
            pltpu.VMEM((MEMBERS, ROWS, WIDTH), jnp.bfloat16),
            pltpu.SemaphoreType.DMA((3, MEMBERS)),
            pltpu.SemaphoreType.DMA((MEMBERS,)),
        ],
        compiler_params=BIG,
        name="rows_pack",
    )(queries, grads, outs, norms)


def relay(block):
    def kernel(block_ref, out_ref):
        out_ref[...] = block_ref[GROUP - FAR2 :]

    return pl.pallas_call(
        kernel,
        in_specs=[VMEM],
        out_specs=VMEM,
        out_shape=jax.ShapeDtypeStruct((FAR2, 2 * HEAD), jnp.bfloat16),
        name="relay",
    )(block)


def attention(doc_lengths, first_token, rows, far2, far1, near, sums, q_far, keys):
    scaling = 1.0 / math.sqrt(HEAD)
    docs = doc_lengths.shape[0]
    parts = TQ // ROWS
    tiles = GROUP // TQ
    pair = 2 * HEAD
    low_row = FAR if keys == "near" else 0
    high_row = FAR if keys == "far" else WINDOW
    held = pl.ds(low_row, high_row - low_row)
    sources = [
        (ref, begin, size)
        for ref, begin, size in ((far2, 0, FAR2), (far1, FAR2, GROUP), (near, FAR, GROUP))
        if low_row <= begin < high_row
    ]
    operands = [doc_lengths, first_token, rows] + [ref for ref, _, _ in sources]
    if keys != "all":
        operands.append(sums)
    if keys == "near":
        operands.append(q_far)

    def kernel(lengths_ref, first_ref, rows_hbm, *rest):
        rest = list(rest)
        source_refs = [rest.pop(0) for _ in sources]
        if keys != "all":
            sums_hbm = rest.pop(0)
        if keys == "near":
            q_far_hbm = rest.pop(0)
        q_hbm = rest.pop(0)
        sums_out = [rest.pop(0) for _ in (sources if keys != "all" else [0])]
        rows_ref, q_ref, window, acc, q_acc, row_sem, key_sem, q_sem, sums_ref, sums_sem, far_sem = rest

        def rows_copy(tile):
            cut = pl.ds(tile * parts, parts)
            return pltpu.make_async_copy(rows_hbm.at[cut], rows_ref.at[cut], row_sem.at[tile])

        def q_copy(tile):
            if keys == "far":
                return pltpu.make_async_copy(q_acc.at[tile], q_hbm.at[tile], q_sem.at[tile])
            cut = pl.ds(tile * parts, parts)
            return pltpu.make_async_copy(q_ref.at[cut], q_hbm.at[cut], q_sem.at[tile])

        def q_far_copy(tile):
            return pltpu.make_async_copy(q_far_hbm.at[tile], q_acc.at[tile], far_sem.at[tile])

        def sums_copy():
            return pltpu.make_async_copy(sums_hbm.at[held], sums_ref.at[held], sums_sem)

        key_copies = [
            pltpu.make_async_copy(ref, window.at[pl.ds(begin, size)], key_sem.at[i])
            for i, (ref, (_, begin, size)) in enumerate(zip(source_refs, sources))
        ]
        for copy in key_copies:
            copy.start()
        for tile in range(tiles):
            rows_copy(tile).start()
            if keys == "near":
                q_far_copy(tile).start()
        if keys != "all":
            sums_copy().start()
        acc[low_row:high_row] = jnp.zeros((high_row - low_row, pair), jnp.float32)
        for copy in key_copies:
            copy.wait()
        group_first = first_ref[0]
        window_first = group_first - FAR

        def query_tile(tile, carry):
            token = group_first + tile * TQ
            position = token + lax.broadcasted_iota(jnp.int32, (8, TQ), 1)
            start = jnp.int32(0)
            doc_first = start
            doc_start = jnp.zeros((8, TQ), jnp.int32)
            for doc in range(1, docs):
                start = start + lengths_ref[doc - 1]
                doc_first = jnp.where(start <= token, start, doc_first)
                doc_start = jnp.where(start <= position, start, doc_start)
            low = doc_start[0:1] - window_first
            reach = position[0:1] - doc_start[0:1]
            key_begin = (doc_first - window_first) // TK
            key_end = (token + TQ - 1 - window_first) // TK + 1
            if keys == "far":
                key_end = jnp.minimum(key_end, FAR // TK)
            if keys == "near":
                key_begin = jnp.maximum(key_begin, FAR // TK)
            block = tile * parts
            rows_copy(tile).wait()
            if keys == "near":
                q_far_copy(tile).wait()
            else:
                q_acc[tile] = jnp.zeros((H * TQ, HEAD), jnp.float32)
            pairs = [(h, s) for h in range(H) for s in range(parts)]
            query = jnp.concatenate(
                [rows_ref[block + s, 0:ROWS, h * HEAD : (h + 1) * HEAD] for h, s in pairs], axis=0
            )
            grad = jnp.concatenate(
                [
                    rows_ref[block + s, 0:ROWS, WIDTH + h * HEAD : WIDTH + (h + 1) * HEAD]
                    for h, s in pairs
                ],
                axis=0,
            )
            stats = [
                sum(
                    rows_ref[block + s, ROWS : ROWS + STATS, t * ROWS : (t + 1) * ROWS].astype(
                        jnp.float32
                    )
                    for t in (2, 1, 0)
                )
                for s in range(parts)
            ]
            norm = LOG2E * jnp.concatenate([stats[s][h : h + 1] for h, s in pairs], axis=1)
            delta = jnp.concatenate([stats[s][H + h : H + h + 1] for h, s in pairs], axis=1)

            def key_tile(index, inner):
                row = pl.multiple_of(index * TK, TK)
                k_rows = window[pl.ds(row, TK), 0:HEAD]
                v_rows = window[pl.ds(row, TK), HEAD : 2 * HEAD]
                offset = row + lax.broadcasted_iota(jnp.int32, (TK, TQ), 0) - low
                allowed = (offset >= 0) & (offset <= reach)
                bias = jnp.concatenate([jnp.where(allowed, 0.0, MASKED)] * H, axis=1)
                scores = lax.dot_general(k_rows, query, NT, preferred_element_type=jnp.float32)
                attend = jnp.exp2(scores * (scaling * LOG2E) - norm + bias)
                prob_grad = lax.dot_general(v_rows, grad, NT, preferred_element_type=jnp.float32)
                score_low = (attend * (prob_grad - delta)).astype(jnp.bfloat16)
                attend_low = attend.astype(jnp.bfloat16)
                acc[pl.ds(row, TK), HEAD : 2 * HEAD] += jnp.dot(
                    attend_low, grad, preferred_element_type=jnp.float32
                )
                acc[pl.ds(row, TK), 0:HEAD] += jnp.dot(
                    score_low, query, preferred_element_type=jnp.float32
                )
                q_acc[tile] += lax.dot_general(
                    score_low, k_rows, TN, preferred_element_type=jnp.float32
                )
                return inner

            lax.fori_loop(key_begin, key_end, key_tile, 0)
            if keys != "far":
                for at_row, (h, s) in enumerate(pairs):
                    part = q_acc[tile, at_row * ROWS : (at_row + 1) * ROWS, :] * scaling
                    q_ref[block + s, :, h * HEAD : (h + 1) * HEAD] = part.astype(jnp.bfloat16)
            q_copy(tile).start()
            return carry

        lax.fori_loop(0, tiles, query_tile, 0)
        if keys == "all":
            pltpu.sync_copy(acc, sums_out[0])
        else:
            sums_copy().wait()
            for ref, (_, begin, size) in zip(sums_out, sources):
                total = acc[begin : begin + size] + sums_ref[begin : begin + size]
                ref[:, 0:HEAD] = (total[:, 0:HEAD] * scaling).astype(ref.dtype)
                ref[:, HEAD : 2 * HEAD] = total[:, HEAD : 2 * HEAD].astype(ref.dtype)
        for tile in range(tiles):
            q_copy(tile).wait()

    q_shape = jax.ShapeDtypeStruct((MEMBERS, ROWS, WIDTH), jnp.bfloat16)
    acc_shape = (WINDOW, pair)
    q_acc_shape = (tiles, H * TQ, HEAD)
    if keys == "all":
        out_shape = [q_shape, jax.ShapeDtypeStruct(acc_shape, jnp.float32)]
        out_specs = [ANY, ANY]
    elif keys == "far":
        out_shape = [jax.ShapeDtypeStruct(q_acc_shape, jnp.float32)]
        out_shape += [jax.ShapeDtypeStruct((size, pair), jnp.bfloat16) for _, _, size in sources]
        out_specs = [ANY] + [VMEM] * len(sources)
    else:
        out_shape = [q_shape, jax.ShapeDtypeStruct((GROUP, pair), jnp.float32)]
        out_specs = [ANY, VMEM]
    return pl.pallas_call(
        kernel,
        in_specs=[SMEM, SMEM] + [ANY] * (len(operands) - 2),
        out_specs=out_specs,
        out_shape=out_shape,
        scratch_shapes=[
            pltpu.VMEM((MEMBERS, ROWS + STATS, 2 * WIDTH), jnp.bfloat16),
            pltpu.VMEM(q_shape.shape, q_shape.dtype),
            pltpu.VMEM((WINDOW, pair), jnp.bfloat16),
            pltpu.VMEM(acc_shape, jnp.float32),
            pltpu.VMEM(q_acc_shape, jnp.float32),
            pltpu.SemaphoreType.DMA((tiles,)),
            pltpu.SemaphoreType.DMA((3,)),
            pltpu.SemaphoreType.DMA((tiles,)),
            pltpu.VMEM(acc_shape, jnp.float32),
            pltpu.SemaphoreType.DMA,
            pltpu.SemaphoreType.DMA((tiles,)),
        ],
        compiler_params=BIG,
    )(*operands)


def kv_sum(member, near, back1, back2):
    skip = (GROUP - FAR2) // ROWS
    wide = 2 * HEAD

    def kernel(member_ref, near_hbm, back1_hbm, back2_hbm, *rest):
        outs, (near_ref, back1_ref, back2_ref, out_ref, sems) = rest[:MEMBERS], rest[MEMBERS:]

        def inbound(k):
            b = (member_ref[0] + k) % MEMBERS
            cut = pl.ds(pl.multiple_of(b * ROWS, ROWS), ROWS)
            far = pl.ds(pl.multiple_of(jnp.maximum(b - skip, 0) * ROWS, ROWS), ROWS)
            return (
                pltpu.make_async_copy(near_hbm.at[cut], near_ref.at[k], sems.at[0, k]),
                pltpu.make_async_copy(back1_hbm.at[cut], back1_ref.at[k], sems.at[1, k]),
                pltpu.make_async_copy(back2_hbm.at[far], back2_ref.at[k], sems.at[2, k]),
            )

        def outbound(k):
            return pltpu.make_async_copy(out_ref.at[k], outs[k], sems.at[3, k])

        for k in range(MEMBERS):
            for copy in inbound(k):
                copy.start()
        for k in range(MEMBERS):
            for copy in inbound(k):
                copy.wait()
            reached = (member_ref[0] + k) % MEMBERS >= skip
            total = near_ref[k] + back1_ref[k].astype(jnp.float32)
            total = total + jnp.where(reached, back2_ref[k].astype(jnp.float32), 0.0)
            out_ref[k] = total.astype(jnp.bfloat16)
            outbound(k).start()
        for k in range(MEMBERS):
            outbound(k).wait()

    shape = (MEMBERS, ROWS, wide)
    return pl.pallas_call(
        kernel,
        in_specs=[SMEM] + [ANY] * 3,
        out_specs=[ANY] * MEMBERS,
        out_shape=[jax.ShapeDtypeStruct((ROWS, wide), jnp.bfloat16)] * MEMBERS,
        scratch_shapes=[
            pltpu.VMEM(shape, jnp.float32),
            pltpu.VMEM(shape, jnp.bfloat16),
            pltpu.VMEM(shape, jnp.bfloat16),
            pltpu.VMEM(shape, jnp.bfloat16),
            pltpu.SemaphoreType.DMA((4, MEMBERS)),
        ],
        compiler_params=BIG,
        name="kv_sum",
    )(member, near, back1, back2)


def q_unpack(parts):
    def kernel(*refs):
        sources, (out_ref, narrow, wide, arrived, sent) = refs[:CHUNKS], refs[CHUNKS:]
        pieces = [(chunk, b) for chunk in range(CHUNKS) for b in range(MEMBERS)]

        def inbound(chunk, b):
            return pltpu.make_async_copy(
                sources[chunk].at[b], narrow.at[chunk, b], arrived.at[chunk, b]
            )

        def outbound(chunk, b):
            cut = pl.ds((b * CHUNKS + chunk) * WIDTH, WIDTH)
            return pltpu.make_async_copy(
                wide.at[chunk, b], out_ref.at[:, cut], sent.at[chunk, b]
            )

        for piece in pieces:
            inbound(*piece).start()
        for chunk, b in pieces:
            inbound(chunk, b).wait()
            wide[chunk, b] = narrow[chunk, b].astype(jnp.float32)
            outbound(chunk, b).start()
        for piece in pieces:
            outbound(*piece).wait()

    shape = (CHUNKS, MEMBERS, ROWS, WIDTH)
    return pl.pallas_call(
        kernel,
        in_specs=[ANY] * CHUNKS,
        out_specs=ANY,
        out_shape=jax.ShapeDtypeStruct((ROWS, MEMBERS * CHUNKS * WIDTH), jnp.float32),
        scratch_shapes=[
            pltpu.VMEM(shape, jnp.bfloat16),
            pltpu.VMEM(shape, jnp.float32),
            pltpu.SemaphoreType.DMA((CHUNKS, MEMBERS)),
            pltpu.SemaphoreType.DMA((CHUNKS, MEMBERS)),
        ],
        compiler_params=BIG,
        name="q_unpack",
    )(*parts)


def kv_unpack(member, pieces):
    def kernel(member_ref, *rest):
        sources, (k_hbm, v_hbm, both_ref, k_ref, v_ref, sems) = rest[:MEMBERS], rest[MEMBERS:]

        def inbound(k):
            return pltpu.make_async_copy(sources[k], both_ref.at[k], sems.at[0, k])

        def outbound(k):
            head = (member_ref[0] + MEMBERS - k) % MEMBERS
            cut = pl.ds(pl.multiple_of(head * HEAD, HEAD), HEAD)
            return (
                pltpu.make_async_copy(k_ref.at[k], k_hbm.at[:, cut], sems.at[1, k]),
                pltpu.make_async_copy(v_ref.at[k], v_hbm.at[:, cut], sems.at[2, k]),
            )

        for k in range(MEMBERS):
            inbound(k).start()
        for k in range(MEMBERS):
            inbound(k).wait()
            k_ref[k] = both_ref[k, :, 0:HEAD].astype(jnp.float32)
            v_ref[k] = both_ref[k, :, HEAD:].astype(jnp.float32)
            for copy in outbound(k):
                copy.start()
        for k in range(MEMBERS):
            for copy in outbound(k):
                copy.wait()

    shape = jax.ShapeDtypeStruct((ROWS, MEMBERS * HEAD), jnp.float32)
    halves = pltpu.VMEM((MEMBERS, ROWS, HEAD), jnp.float32)
    return pl.pallas_call(
        kernel,
        in_specs=[SMEM] + [ANY] * MEMBERS,
        out_specs=[ANY, ANY],
        out_shape=[shape, shape],
        scratch_shapes=[
            pltpu.VMEM((MEMBERS, ROWS, 2 * HEAD), jnp.bfloat16),
            halves,
            halves,
            pltpu.SemaphoreType.DMA((3, MEMBERS)),
        ],
        compiler_params=BIG,
        name="kv_unpack",
    )(member, *pieces)


def exchange(blocks):
    return lax.all_to_all(blocks, ("core", "head"), split_axis=0, concat_axis=0, tiled=True)


def shifted(block, by):
    count = lax.axis_size("group")
    pairs = [(i, i + by) for i in range(count) if 0 <= i + by < count]
    return lax.ppermute(block, "group", pairs)


def on_device(queries, keys, values, out_rows, output_gradient, log_norm_rows, doc_lengths):
    near = exchange(kv_pack(keys, values)).reshape(GROUP, 2 * HEAD)
    norms = log_norm_rows.T
    rows = []
    for chunk in range(CHUNKS):
        packed = rows_pack(queries, output_gradient, out_rows, norms, chunk)
        rows.append(exchange(packed))
    far1 = shifted(near, 1)
    relayed = relay(far1)
    far2 = shifted(relayed, 1)
    first_token = (lax.axis_index("group") * GROUP).astype(jnp.int32).reshape(1)
    member = lax.axis_index(("core", "head")).astype(jnp.int32).reshape(1)
    fixed = (doc_lengths, first_token)
    q_part, sums = attention(*fixed, rows[0], far2, far1, near, None, None, "all")
    q_back = [exchange(q_part)]
    q_far, far2_sum, far1_sum = attention(*fixed, rows[1], far2, far1, near, sums, None, "far")
    back1 = shifted(far1_sum, -1)
    back2 = shifted(far2_sum, -2)
    q_part, near_sum = attention(
        *fixed, rows[1], far2, far1, near, sums, q_far, "near"
    )
    q_back.append(exchange(q_part))
    pieces = list(kv_sum(member, near_sum, back1, back2))
    for k in range(1, MEMBERS):
        ring = [(i, (i + k) % MEMBERS) for i in range(MEMBERS)]
        pieces[k] = lax.ppermute(pieces[k], ("core", "head"), ring)
    key_gradient, value_gradient = kv_unpack(member, pieces)
    q_grad = q_unpack(q_back)
    return (q_grad, key_gradient, value_gradient)


def solution(mesh):
    wide, head = mesh.shape["wide"], mesh.shape["head"]
    cores = MEMBERS // head
    finer = Mesh(mesh.devices.reshape(wide // cores, cores, head), ("group", "core", "head"))
    split = P(("group", "core", "head"), None)
    return jax.shard_map(
        on_device,
        mesh=finer,
        in_specs=(split,) * 6 + (P(),),
        out_specs=(split, split, split),
        check_vma=False,
    )
```

```python
import math

import jax
import jax.numpy as jnp
from jax import lax
from jax.experimental import pallas as pl
from jax.experimental.pallas import tpu as pltpu
from jax.sharding import Mesh, PartitionSpec as P


LOG2E = math.log2(math.e)
MASKED = -1e30
HEAD = 128
ROWS = 128
MEMBERS = 8
GROUP = MEMBERS * ROWS
FAR_BLOCKS = 14
FAR = FAR_BLOCKS * ROWS
FAR2 = FAR - GROUP
WINDOW = FAR + GROUP
HEADS = 8
CHUNKS = 2
H = HEADS // CHUNKS
WIDTH = H * HEAD
STATS = 2 * H
TQ = 256
TK = 256
NT = (((1,), (1,)), ((), ()))
TN = (((0,), (0,)), ((), ()))

SMEM = pl.BlockSpec(memory_space=pltpu.SMEM)
VMEM = pl.BlockSpec(memory_space=pltpu.VMEM)
ANY = pl.BlockSpec(memory_space=pl.ANY)
BIG = pltpu.CompilerParams(vmem_limit_bytes=56 << 20)


def kv_pack(keys, values):
    def kernel(k_ref, v_ref, out_ref):
        for b in range(MEMBERS):
            out_ref[b, :, 0:HEAD] = k_ref[:, b * HEAD : (b + 1) * HEAD]
            out_ref[b, :, HEAD : 2 * HEAD] = v_ref[:, b * HEAD : (b + 1) * HEAD]

    return pl.pallas_call(
        kernel,
        in_specs=[VMEM, VMEM],
        out_specs=VMEM,
        out_shape=jax.ShapeDtypeStruct((MEMBERS, ROWS, 2 * HEAD), jnp.bfloat16),
        name="kv_pack",
    )(keys, values)


def split_terms(value):
    high = value.astype(jnp.bfloat16)
    rest = value - high.astype(jnp.float32)
    middle = rest.astype(jnp.bfloat16)
    low = (rest - middle.astype(jnp.float32)).astype(jnp.bfloat16)
    return high, middle, low


def rows_pack(queries, grads, outs, norms, chunk):
    def kernel(q_ref, g_ref, o_ref, n_ref, out_ref, packed, forward, arrived, sent):
        def inbound(b):
            cut = pl.ds((b * CHUNKS + chunk) * WIDTH, WIDTH)
            return (
                pltpu.make_async_copy(
                    q_ref.at[:, cut], packed.at[b, pl.ds(0, ROWS), pl.ds(0, WIDTH)], arrived.at[0, b]
                ),
                pltpu.make_async_copy(
                    g_ref.at[:, cut],
                    packed.at[b, pl.ds(0, ROWS), pl.ds(WIDTH, WIDTH)],
                    arrived.at[1, b],
                ),
                pltpu.make_async_copy(o_ref.at[:, cut], forward.at[b], arrived.at[2, b]),
            )

        for b in range(MEMBERS):
            for copy in inbound(b):
                copy.start()
        lane = lax.broadcasted_iota(jnp.int32, (ROWS, 128), 1)
        for b in range(MEMBERS):
            for copy in inbound(b):
                copy.wait()
            deltas = jnp.zeros((ROWS, 128), jnp.float32)
            for h in range(H):
                cut = slice(h * HEAD, (h + 1) * HEAD)
                grad = packed[b, 0:ROWS, WIDTH + h * HEAD : WIDTH + (h + 1) * HEAD]
                product = grad.astype(jnp.float32) * forward[b, :, cut].astype(jnp.float32)
                deltas = jnp.where(lane == h, jnp.sum(product, axis=1, keepdims=True), deltas)
            first = b * HEADS + chunk * H
            stats = jnp.concatenate([n_ref[first : first + H], deltas.T[0:H]], axis=0)
            high, middle, low = split_terms(stats)
            packed[b, ROWS : ROWS + STATS, 0:ROWS] = high
            packed[b, ROWS : ROWS + STATS, ROWS : 2 * ROWS] = middle
            packed[b, ROWS : ROWS + STATS, 2 * ROWS : 3 * ROWS] = low
            packed[b, ROWS : ROWS + STATS, 3 * ROWS :] = jnp.zeros(
                (STATS, 2 * WIDTH - 3 * ROWS), jnp.bfloat16
            )
            pltpu.make_async_copy(packed.at[b], out_ref.at[b], sent.at[b]).start()
        for b in range(MEMBERS):
            pltpu.make_async_copy(packed.at[b], out_ref.at[b], sent.at[b]).wait()

    shape = (MEMBERS, ROWS + STATS, 2 * WIDTH)
    return pl.pallas_call(
        kernel,
        in_specs=[ANY, ANY, ANY, VMEM],
        out_specs=ANY,
        out_shape=jax.ShapeDtypeStruct(shape, jnp.bfloat16),
        scratch_shapes=[
            pltpu.VMEM(shape, jnp.bfloat16),
            pltpu.VMEM((MEMBERS, ROWS, WIDTH), jnp.bfloat16),
            pltpu.SemaphoreType.DMA((3, MEMBERS)),
            pltpu.SemaphoreType.DMA((MEMBERS,)),
        ],
        compiler_params=BIG,
        name="rows_pack",
    )(queries, grads, outs, norms)


def attention(doc_lengths, first_token, rows, far2, far1, near, sums, q_far, keys):
    scaling = 1.0 / math.sqrt(HEAD)
    docs = doc_lengths.shape[0]
    parts = TQ // ROWS
    tiles = GROUP // TQ
    pair = 2 * HEAD
    low_row = FAR if keys == "near" else 0
    high_row = FAR if keys == "far" else WINDOW
    held = pl.ds(low_row, high_row - low_row)
    sources = [
        (ref, begin, ref.shape[0])
        for ref, begin in zip(
            (far2, *far1, near), (0, FAR2, FAR2 + far1[0].shape[0], FAR)
        )
        if low_row <= begin < high_row
    ]
    targets = {"all": [(0, WINDOW)], "far": [(0, FAR2), (FAR2, GROUP)], "near": [(FAR, GROUP)]}[keys]
    operands = [doc_lengths, first_token, rows] + [ref for ref, _, _ in sources]
    if keys != "all":
        operands.append(sums)
    if keys == "near":
        operands.append(q_far)

    def kernel(lengths_ref, first_ref, rows_hbm, *rest):
        rest = list(rest)
        source_refs = [rest.pop(0) for _ in sources]
        if keys != "all":
            sums_hbm = rest.pop(0)
        if keys == "near":
            q_far_hbm = rest.pop(0)
        q_hbm = rest.pop(0)
        sums_out = [rest.pop(0) for _ in targets]
        rows_ref, q_ref, window, acc, q_acc, row_sem, key_sem, q_sem, sums_ref, sums_sem, far_sem = rest

        def rows_copy(tile):
            cut = pl.ds(tile * parts, parts)
            return pltpu.make_async_copy(rows_hbm.at[cut], rows_ref.at[cut], row_sem.at[tile])

        def q_copy(tile):
            if keys == "far":
                return pltpu.make_async_copy(q_acc.at[tile], q_hbm.at[tile], q_sem.at[tile])
            cut = pl.ds(tile * parts, parts)
            return pltpu.make_async_copy(q_ref.at[cut], q_hbm.at[cut], q_sem.at[tile])

        def q_far_copy(tile):
            return pltpu.make_async_copy(q_far_hbm.at[tile], q_acc.at[tile], far_sem.at[tile])

        def sums_copy():
            return pltpu.make_async_copy(sums_hbm.at[held], sums_ref.at[held], sums_sem)

        key_copies = [
            pltpu.make_async_copy(ref, window.at[pl.ds(begin, size)], key_sem.at[i])
            for i, (ref, (_, begin, size)) in enumerate(zip(source_refs, sources))
        ]
        for copy in key_copies:
            copy.start()
        for tile in range(tiles):
            rows_copy(tile).start()
            if keys == "near":
                q_far_copy(tile).start()
        if keys != "all":
            sums_copy().start()
        acc[low_row:high_row] = jnp.zeros((high_row - low_row, pair), jnp.float32)
        for copy in key_copies:
            copy.wait()
        group_first = first_ref[0]
        window_first = group_first - FAR

        def query_tile(tile, carry):
            token = group_first + tile * TQ
            position = token + lax.broadcasted_iota(jnp.int32, (8, TQ), 1)
            start = jnp.int32(0)
            doc_first = start
            doc_start = jnp.zeros((8, TQ), jnp.int32)
            for doc in range(1, docs):
                start = start + lengths_ref[doc - 1]
                doc_first = jnp.where(start <= token, start, doc_first)
                doc_start = jnp.where(start <= position, start, doc_start)
            low = doc_start[0:1] - window_first
            reach = position[0:1] - doc_start[0:1]
            key_begin = (doc_first - window_first) // TK
            key_end = (token + TQ - 1 - window_first) // TK + 1
            if keys == "far":
                key_end = jnp.minimum(key_end, FAR // TK)
            if keys == "near":
                key_begin = jnp.maximum(key_begin, FAR // TK)
            block = tile * parts
            rows_copy(tile).wait()
            if keys == "near":
                q_far_copy(tile).wait()
            else:
                q_acc[tile] = jnp.zeros((H * TQ, HEAD), jnp.float32)
            pairs = [(h, s) for h in range(H) for s in range(parts)]
            query = jnp.concatenate(
                [rows_ref[block + s, 0:ROWS, h * HEAD : (h + 1) * HEAD] for h, s in pairs], axis=0
            )
            grad = jnp.concatenate(
                [
                    rows_ref[block + s, 0:ROWS, WIDTH + h * HEAD : WIDTH + (h + 1) * HEAD]
                    for h, s in pairs
                ],
                axis=0,
            )
            stats = [
                sum(
                    rows_ref[block + s, ROWS : ROWS + STATS, t * ROWS : (t + 1) * ROWS].astype(
                        jnp.float32
                    )
                    for t in (2, 1, 0)
                )
                for s in range(parts)
            ]
            norm = LOG2E * jnp.concatenate([stats[s][h : h + 1] for h, s in pairs], axis=1)
            delta = jnp.concatenate([stats[s][H + h : H + h + 1] for h, s in pairs], axis=1)

            def key_tile(index, inner):
                row = pl.multiple_of(index * TK, TK)
                k_rows = window[pl.ds(row, TK), 0:HEAD]
                v_rows = window[pl.ds(row, TK), HEAD : 2 * HEAD]
                offset = row + lax.broadcasted_iota(jnp.int32, (TK, TQ), 0) - low
                allowed = (offset >= 0) & (offset <= reach)
                bias = jnp.concatenate([jnp.where(allowed, 0.0, MASKED)] * H, axis=1)
                scores = lax.dot_general(k_rows, query, NT, preferred_element_type=jnp.float32)
                attend = jnp.exp2(scores * (scaling * LOG2E) - norm + bias)
                prob_grad = lax.dot_general(v_rows, grad, NT, preferred_element_type=jnp.float32)
                score_low = (attend * (prob_grad - delta)).astype(jnp.bfloat16)
                attend_low = attend.astype(jnp.bfloat16)
                acc[pl.ds(row, TK), HEAD : 2 * HEAD] += jnp.dot(
                    attend_low, grad, preferred_element_type=jnp.float32
                )
                acc[pl.ds(row, TK), 0:HEAD] += jnp.dot(
                    score_low, query, preferred_element_type=jnp.float32
                )
                q_acc[tile] += lax.dot_general(
                    score_low, k_rows, TN, preferred_element_type=jnp.float32
                )
                return inner

            def two_tiles(index, inner):
                key_tile(key_begin + 2 * index, inner)
                return key_tile(key_begin + 2 * index + 1, inner)

            twos = jnp.maximum(key_end - key_begin, 0) // 2
            lax.fori_loop(0, twos, two_tiles, 0)
            lax.fori_loop(key_begin + 2 * twos, key_end, key_tile, 0)
            if keys != "far":
                for at_row, (h, s) in enumerate(pairs):
                    part = q_acc[tile, at_row * ROWS : (at_row + 1) * ROWS, :] * scaling
                    q_ref[block + s, :, h * HEAD : (h + 1) * HEAD] = part.astype(jnp.bfloat16)
            q_copy(tile).start()
            return carry

        lax.fori_loop(0, tiles, query_tile, 0)
        if keys == "all":
            pltpu.sync_copy(acc, sums_out[0])
        else:
            sums_copy().wait()
            for ref, (begin, size) in zip(sums_out, targets):
                total = acc[begin : begin + size] + sums_ref[begin : begin + size]
                ref[:, 0:HEAD] = (total[:, 0:HEAD] * scaling).astype(ref.dtype)
                ref[:, HEAD : 2 * HEAD] = total[:, HEAD : 2 * HEAD].astype(ref.dtype)
        for tile in range(tiles):
            q_copy(tile).wait()

    q_shape = jax.ShapeDtypeStruct((MEMBERS, ROWS, WIDTH), jnp.bfloat16)
    acc_shape = (WINDOW, pair)
    q_acc_shape = (tiles, H * TQ, HEAD)
    if keys == "all":
        out_shape = [q_shape, jax.ShapeDtypeStruct(acc_shape, jnp.float32)]
        out_specs = [ANY, ANY]
    elif keys == "far":
        out_shape = [jax.ShapeDtypeStruct(q_acc_shape, jnp.float32)]
        out_shape += [jax.ShapeDtypeStruct((size, pair), jnp.bfloat16) for _, size in targets]
        out_specs = [ANY] + [VMEM] * len(targets)
    else:
        out_shape = [q_shape, jax.ShapeDtypeStruct((GROUP, pair), jnp.float32)]
        out_specs = [ANY, VMEM]
    return pl.pallas_call(
        kernel,
        in_specs=[SMEM, SMEM] + [ANY] * (len(operands) - 2),
        out_specs=out_specs,
        out_shape=out_shape,
        scratch_shapes=[
            pltpu.VMEM((MEMBERS, ROWS + STATS, 2 * WIDTH), jnp.bfloat16),
            pltpu.VMEM(q_shape.shape, q_shape.dtype),
            pltpu.VMEM((WINDOW, pair), jnp.bfloat16),
            pltpu.VMEM(acc_shape, jnp.float32),
            pltpu.VMEM(q_acc_shape, jnp.float32),
            pltpu.SemaphoreType.DMA((tiles,)),
            pltpu.SemaphoreType.DMA((4,)),
            pltpu.SemaphoreType.DMA((tiles,)),
            pltpu.VMEM(acc_shape, jnp.float32),
            pltpu.SemaphoreType.DMA,
            pltpu.SemaphoreType.DMA((tiles,)),
        ],
        compiler_params=BIG,
    )(*operands)


def kv_sum(member, near, back1, back2):
    skip = (GROUP - FAR2) // ROWS
    wide = 2 * HEAD

    def kernel(member_ref, near_hbm, back1_hbm, back2_hbm, *rest):
        outs, (near_ref, back1_ref, back2_ref, out_ref, sems) = rest[:MEMBERS], rest[MEMBERS:]

        def inbound(k):
            b = (member_ref[0] + k) % MEMBERS
            cut = pl.ds(pl.multiple_of(b * ROWS, ROWS), ROWS)
            far = pl.ds(pl.multiple_of(jnp.maximum(b - skip, 0) * ROWS, ROWS), ROWS)
            return (
                pltpu.make_async_copy(near_hbm.at[cut], near_ref.at[k], sems.at[0, k]),
                pltpu.make_async_copy(back1_hbm.at[cut], back1_ref.at[k], sems.at[1, k]),
                pltpu.make_async_copy(back2_hbm.at[far], back2_ref.at[k], sems.at[2, k]),
            )

        def outbound(k):
            return pltpu.make_async_copy(out_ref.at[k], outs[k], sems.at[3, k])

        for k in range(MEMBERS):
            for copy in inbound(k):
                copy.start()
        for k in range(MEMBERS):
            for copy in inbound(k):
                copy.wait()
            reached = (member_ref[0] + k) % MEMBERS >= skip
            total = near_ref[k] + back1_ref[k].astype(jnp.float32)
            total = total + jnp.where(reached, back2_ref[k].astype(jnp.float32), 0.0)
            out_ref[k] = total.astype(jnp.bfloat16)
            outbound(k).start()
        for k in range(MEMBERS):
            outbound(k).wait()

    shape = (MEMBERS, ROWS, wide)
    return pl.pallas_call(
        kernel,
        in_specs=[SMEM] + [ANY] * 3,
        out_specs=[ANY] * MEMBERS,
        out_shape=[jax.ShapeDtypeStruct((ROWS, wide), jnp.bfloat16)] * MEMBERS,
        scratch_shapes=[
            pltpu.VMEM(shape, jnp.float32),
            pltpu.VMEM(shape, jnp.bfloat16),
            pltpu.VMEM(shape, jnp.bfloat16),
            pltpu.VMEM(shape, jnp.bfloat16),
            pltpu.SemaphoreType.DMA((4, MEMBERS)),
        ],
        compiler_params=BIG,
        name="kv_sum",
    )(member, near, back1, back2)


def q_unpack(parts):
    def kernel(*refs):
        sources, (out_ref, narrow, wide, arrived, sent) = refs[:CHUNKS], refs[CHUNKS:]
        pieces = [(chunk, b) for chunk in range(CHUNKS) for b in range(MEMBERS)]

        def inbound(chunk, b):
            return pltpu.make_async_copy(
                sources[chunk].at[b], narrow.at[chunk, b], arrived.at[chunk, b]
            )

        def outbound(chunk, b):
            cut = pl.ds((b * CHUNKS + chunk) * WIDTH, WIDTH)
            return pltpu.make_async_copy(
                wide.at[chunk, b], out_ref.at[:, cut], sent.at[chunk, b]
            )

        for piece in pieces:
            inbound(*piece).start()
        for chunk, b in pieces:
            inbound(chunk, b).wait()
            wide[chunk, b] = narrow[chunk, b].astype(jnp.float32)
            outbound(chunk, b).start()
        for piece in pieces:
            outbound(*piece).wait()

    shape = (CHUNKS, MEMBERS, ROWS, WIDTH)
    return pl.pallas_call(
        kernel,
        in_specs=[ANY] * CHUNKS,
        out_specs=ANY,
        out_shape=jax.ShapeDtypeStruct((ROWS, MEMBERS * CHUNKS * WIDTH), jnp.float32),
        scratch_shapes=[
            pltpu.VMEM(shape, jnp.bfloat16),
            pltpu.VMEM(shape, jnp.float32),
            pltpu.SemaphoreType.DMA((CHUNKS, MEMBERS)),
            pltpu.SemaphoreType.DMA((CHUNKS, MEMBERS)),
        ],
        compiler_params=BIG,
        name="q_unpack",
    )(*parts)


def kv_unpack(member, pieces):
    def kernel(member_ref, *rest):
        sources, (k_hbm, v_hbm, both_ref, k_ref, v_ref, sems) = rest[:MEMBERS], rest[MEMBERS:]

        def inbound(k):
            return pltpu.make_async_copy(sources[k], both_ref.at[k], sems.at[0, k])

        def outbound(k):
            head = (member_ref[0] + MEMBERS - k) % MEMBERS
            cut = pl.ds(pl.multiple_of(head * HEAD, HEAD), HEAD)
            return (
                pltpu.make_async_copy(k_ref.at[k], k_hbm.at[:, cut], sems.at[1, k]),
                pltpu.make_async_copy(v_ref.at[k], v_hbm.at[:, cut], sems.at[2, k]),
            )

        for k in range(MEMBERS):
            inbound(k).start()
        for k in range(MEMBERS):
            inbound(k).wait()
            k_ref[k] = both_ref[k, :, 0:HEAD].astype(jnp.float32)
            v_ref[k] = both_ref[k, :, HEAD:].astype(jnp.float32)
            for copy in outbound(k):
                copy.start()
        for k in range(MEMBERS):
            for copy in outbound(k):
                copy.wait()

    shape = jax.ShapeDtypeStruct((ROWS, MEMBERS * HEAD), jnp.float32)
    halves = pltpu.VMEM((MEMBERS, ROWS, HEAD), jnp.float32)
    return pl.pallas_call(
        kernel,
        in_specs=[SMEM] + [ANY] * MEMBERS,
        out_specs=[ANY, ANY],
        out_shape=[shape, shape],
        scratch_shapes=[
            pltpu.VMEM((MEMBERS, ROWS, 2 * HEAD), jnp.bfloat16),
            halves,
            halves,
            pltpu.SemaphoreType.DMA((3, MEMBERS)),
        ],
        compiler_params=BIG,
        name="kv_unpack",
    )(member, *pieces)


def exchange(blocks):
    return lax.all_to_all(blocks, ("core", "head"), split_axis=0, concat_axis=0, tiled=True)


def shifted(block, by):
    count = lax.axis_size("group")
    pairs = [(i, i + by) for i in range(count) if 0 <= i + by < count]
    return lax.ppermute(block, "group", pairs)


def on_device(queries, keys, values, out_rows, output_gradient, log_norm_rows, doc_lengths):
    near = exchange(kv_pack(keys, values)).reshape(GROUP, 2 * HEAD)
    norms = log_norm_rows.T
    rows = []
    for chunk in range(CHUNKS):
        packed = rows_pack(queries, output_gradient, out_rows, norms, chunk)
        rows.append(exchange(packed))
    forwarded = shifted(near[GROUP - FAR2 :], 1)
    far1 = (shifted(near[: GROUP - FAR2], 1), forwarded)
    far2 = shifted(forwarded, 1)
    first_token = (lax.axis_index("group") * GROUP).astype(jnp.int32).reshape(1)
    member = lax.axis_index(("core", "head")).astype(jnp.int32).reshape(1)
    fixed = (doc_lengths, first_token)
    q_part, sums = attention(*fixed, rows[0], far2, far1, near, None, None, "all")
    q_back = [exchange(q_part)]
    q_far, far2_sum, far1_sum = attention(*fixed, rows[1], far2, far1, near, sums, None, "far")
    back1 = shifted(far1_sum, -1)
    back2 = shifted(far2_sum, -2)
    q_part, near_sum = attention(
        *fixed, rows[1], far2, far1, near, sums, q_far, "near"
    )
    q_back.append(exchange(q_part))
    pieces = list(kv_sum(member, near_sum, back1, back2))
    for k in range(1, MEMBERS):
        ring = [(i, (i + k) % MEMBERS) for i in range(MEMBERS)]
        pieces[k] = lax.ppermute(pieces[k], ("core", "head"), ring)
    key_gradient, value_gradient = kv_unpack(member, pieces)
    q_grad = q_unpack(q_back)
    return (q_grad, key_gradient, value_gradient)


def solution(mesh):
    wide, head = mesh.shape["wide"], mesh.shape["head"]
    cores = MEMBERS // head
    finer = Mesh(mesh.devices.reshape(wide // cores, cores, head), ("group", "core", "head"))
    split = P(("group", "core", "head"), None)
    return jax.shard_map(
        on_device,
        mesh=finer,
        in_specs=(split,) * 6 + (P(),),
        out_specs=(split, split, split),
        check_vma=False,
    )
```

```python
import math

import jax
import jax.numpy as jnp
from jax import lax
from jax.experimental import pallas as pl
from jax.experimental.pallas import tpu as pltpu
from jax.sharding import Mesh, PartitionSpec as P


LOG2E = math.log2(math.e)
MASKED = -1e30
HEAD = 128
ROWS = 128
MEMBERS = 8
GROUP = MEMBERS * ROWS
FAR_BLOCKS = 14
FAR = FAR_BLOCKS * ROWS
FAR2 = FAR - GROUP
WINDOW = FAR + GROUP
HEADS = 8
CHUNKS = 2
H = HEADS // CHUNKS
WIDTH = H * HEAD
STATS = 2 * H
STEP = {"all": 2, "far": 3, "near": 2}
TQ = 256
TK = 256
NT = (((1,), (1,)), ((), ()))
TN = (((0,), (0,)), ((), ()))

SMEM = pl.BlockSpec(memory_space=pltpu.SMEM)
VMEM = pl.BlockSpec(memory_space=pltpu.VMEM)
ANY = pl.BlockSpec(memory_space=pl.ANY)
BIG = pltpu.CompilerParams(vmem_limit_bytes=56 << 20)


def kv_pack(keys, values):
    def kernel(k_ref, v_ref, out_ref):
        for b in range(MEMBERS):
            out_ref[b, :, 0:HEAD] = k_ref[:, b * HEAD : (b + 1) * HEAD]
            out_ref[b, :, HEAD : 2 * HEAD] = v_ref[:, b * HEAD : (b + 1) * HEAD]

    return pl.pallas_call(
        kernel,
        in_specs=[VMEM, VMEM],
        out_specs=VMEM,
        out_shape=jax.ShapeDtypeStruct((MEMBERS, ROWS, 2 * HEAD), jnp.bfloat16),
        name="kv_pack",
    )(keys, values)


def split_terms(value):
    high = value.astype(jnp.bfloat16)
    rest = value - high.astype(jnp.float32)
    middle = rest.astype(jnp.bfloat16)
    low = (rest - middle.astype(jnp.float32)).astype(jnp.bfloat16)
    return high, middle, low


def rows_pack(queries, grads, outs, norms, chunk):
    def kernel(q_ref, g_ref, o_ref, n_ref, out_ref, packed, forward, arrived, sent):
        def inbound(b):
            cut = pl.ds((b * CHUNKS + chunk) * WIDTH, WIDTH)
            return (
                pltpu.make_async_copy(
                    q_ref.at[:, cut], packed.at[b, pl.ds(0, ROWS), pl.ds(0, WIDTH)], arrived.at[0, b]
                ),
                pltpu.make_async_copy(
                    g_ref.at[:, cut],
                    packed.at[b, pl.ds(0, ROWS), pl.ds(WIDTH, WIDTH)],
                    arrived.at[1, b],
                ),
                pltpu.make_async_copy(o_ref.at[:, cut], forward.at[b], arrived.at[2, b]),
            )

        for b in range(MEMBERS):
            for copy in inbound(b):
                copy.start()
        lane = lax.broadcasted_iota(jnp.int32, (ROWS, 128), 1)
        for b in range(MEMBERS):
            for copy in inbound(b):
                copy.wait()
            deltas = jnp.zeros((ROWS, 128), jnp.float32)
            for h in range(H):
                cut = slice(h * HEAD, (h + 1) * HEAD)
                grad = packed[b, 0:ROWS, WIDTH + h * HEAD : WIDTH + (h + 1) * HEAD]
                product = grad.astype(jnp.float32) * forward[b, :, cut].astype(jnp.float32)
                deltas = jnp.where(lane == h, jnp.sum(product, axis=1, keepdims=True), deltas)
            first = b * HEADS + chunk * H
            stats = jnp.concatenate([n_ref[first : first + H], deltas.T[0:H]], axis=0)
            high, middle, low = split_terms(stats)
            packed[b, ROWS : ROWS + STATS, 0:ROWS] = high
            packed[b, ROWS : ROWS + STATS, ROWS : 2 * ROWS] = middle
            packed[b, ROWS : ROWS + STATS, 2 * ROWS : 3 * ROWS] = low
            packed[b, ROWS : ROWS + STATS, 3 * ROWS :] = jnp.zeros(
                (STATS, 2 * WIDTH - 3 * ROWS), jnp.bfloat16
            )
            pltpu.make_async_copy(packed.at[b], out_ref.at[b], sent.at[b]).start()
        for b in range(MEMBERS):
            pltpu.make_async_copy(packed.at[b], out_ref.at[b], sent.at[b]).wait()

    shape = (MEMBERS, ROWS + STATS, 2 * WIDTH)
    return pl.pallas_call(
        kernel,
        in_specs=[ANY, ANY, ANY, VMEM],
        out_specs=ANY,
        out_shape=jax.ShapeDtypeStruct(shape, jnp.bfloat16),
        scratch_shapes=[
            pltpu.VMEM(shape, jnp.bfloat16),
            pltpu.VMEM((MEMBERS, ROWS, WIDTH), jnp.bfloat16),
            pltpu.SemaphoreType.DMA((3, MEMBERS)),
            pltpu.SemaphoreType.DMA((MEMBERS,)),
        ],
        compiler_params=BIG,
        name="rows_pack",
    )(queries, grads, outs, norms)


def attention(doc_lengths, first_token, rows, far2, far1, near, sums, q_far, keys):
    scaling = 1.0 / math.sqrt(HEAD)
    docs = doc_lengths.shape[0]
    parts = TQ // ROWS
    tiles = GROUP // TQ
    pair = 2 * HEAD
    low_row = FAR if keys == "near" else 0
    high_row = FAR if keys == "far" else WINDOW
    held = pl.ds(low_row, high_row - low_row)
    sources = [
        (ref, begin, ref.shape[0])
        for ref, begin in zip(
            (far2, *far1, near), (0, FAR2, FAR2 + far1[0].shape[0], FAR)
        )
        if low_row <= begin < high_row
    ]
    targets = {"all": [(0, WINDOW)], "far": [(0, FAR2), (FAR2, GROUP)], "near": [(FAR, GROUP)]}[keys]
    operands = [doc_lengths, first_token, rows] + [ref for ref, _, _ in sources]
    if keys != "all":
        operands.append(sums)
    if keys == "near":
        operands.append(q_far)

    def kernel(lengths_ref, first_ref, rows_hbm, *rest):
        rest = list(rest)
        source_refs = [rest.pop(0) for _ in sources]
        if keys != "all":
            sums_hbm = rest.pop(0)
        if keys == "near":
            q_far_hbm = rest.pop(0)
        q_hbm = rest.pop(0)
        sums_out = [rest.pop(0) for _ in targets]
        rows_ref, q_ref, window, acc, q_acc, row_sem, key_sem, q_sem, sums_ref, sums_sem, far_sem = rest

        def rows_copy(tile):
            cut = pl.ds(tile * parts, parts)
            return pltpu.make_async_copy(rows_hbm.at[cut], rows_ref.at[cut], row_sem.at[tile])

        def q_copy(tile):
            if keys == "far":
                return pltpu.make_async_copy(q_acc.at[tile], q_hbm.at[tile], q_sem.at[tile])
            cut = pl.ds(tile * parts, parts)
            return pltpu.make_async_copy(q_ref.at[cut], q_hbm.at[cut], q_sem.at[tile])

        def q_far_copy(tile):
            return pltpu.make_async_copy(q_far_hbm.at[tile], q_acc.at[tile], far_sem.at[tile])

        def sums_copy():
            return pltpu.make_async_copy(sums_hbm.at[held], sums_ref.at[held], sums_sem)

        key_copies = [
            pltpu.make_async_copy(ref, window.at[pl.ds(begin, size)], key_sem.at[i])
            for i, (ref, (_, begin, size)) in enumerate(zip(source_refs, sources))
        ]
        for copy in key_copies:
            copy.start()
        for tile in range(tiles):
            rows_copy(tile).start()
            if keys == "near":
                q_far_copy(tile).start()
        if keys != "all":
            sums_copy().start()
        acc[low_row:high_row] = jnp.zeros((high_row - low_row, pair), jnp.float32)
        for copy in key_copies:
            copy.wait()
        group_first = first_ref[0]
        window_first = group_first - FAR

        def query_tile(tile, carry):
            token = group_first + tile * TQ
            position = token + lax.broadcasted_iota(jnp.int32, (8, TQ), 1)
            start = jnp.int32(0)
            doc_first = start
            doc_start = jnp.zeros((8, TQ), jnp.int32)
            for doc in range(1, docs):
                start = start + lengths_ref[doc - 1]
                doc_first = jnp.where(start <= token, start, doc_first)
                doc_start = jnp.where(start <= position, start, doc_start)
            low = doc_start[0:1] - window_first
            reach = position[0:1] - doc_start[0:1]
            key_begin = (doc_first - window_first) // TK
            key_end = (token + TQ - 1 - window_first) // TK + 1
            if keys == "far":
                key_end = jnp.minimum(key_end, FAR // TK)
            if keys == "near":
                key_begin = jnp.maximum(key_begin, FAR // TK)
            block = tile * parts
            rows_copy(tile).wait()
            if keys == "near":
                q_far_copy(tile).wait()
            else:
                q_acc[tile] = jnp.zeros((H * TQ, HEAD), jnp.float32)
            pairs = [(h, s) for h in range(H) for s in range(parts)]
            query = jnp.concatenate(
                [rows_ref[block + s, 0:ROWS, h * HEAD : (h + 1) * HEAD] for h, s in pairs], axis=0
            )
            grad = jnp.concatenate(
                [
                    rows_ref[block + s, 0:ROWS, WIDTH + h * HEAD : WIDTH + (h + 1) * HEAD]
                    for h, s in pairs
                ],
                axis=0,
            )
            stats = [
                sum(
                    rows_ref[block + s, ROWS : ROWS + STATS, t * ROWS : (t + 1) * ROWS].astype(
                        jnp.float32
                    )
                    for t in (2, 1, 0)
                )
                for s in range(parts)
            ]
            norm = LOG2E * jnp.concatenate([stats[s][h : h + 1] for h, s in pairs], axis=1)
            delta = jnp.concatenate([stats[s][H + h : H + h + 1] for h, s in pairs], axis=1)

            def key_tile(index, inner):
                row = pl.multiple_of(index * TK, TK)
                k_rows = window[pl.ds(row, TK), 0:HEAD]
                v_rows = window[pl.ds(row, TK), HEAD : 2 * HEAD]
                offset = row + lax.broadcasted_iota(jnp.int32, (TK, TQ), 0) - low
                allowed = (offset >= 0) & (offset <= reach)
                bias = jnp.concatenate([jnp.where(allowed, 0.0, MASKED)] * H, axis=1)
                scores = lax.dot_general(k_rows, query, NT, preferred_element_type=jnp.float32)
                attend = jnp.exp2(scores * (scaling * LOG2E) - norm + bias)
                prob_grad = lax.dot_general(v_rows, grad, NT, preferred_element_type=jnp.float32)
                score_low = (attend * (prob_grad - delta)).astype(jnp.bfloat16)
                attend_low = attend.astype(jnp.bfloat16)
                acc[pl.ds(row, TK), HEAD : 2 * HEAD] += jnp.dot(
                    attend_low, grad, preferred_element_type=jnp.float32
                )
                acc[pl.ds(row, TK), 0:HEAD] += jnp.dot(
                    score_low, query, preferred_element_type=jnp.float32
                )
                q_acc[tile] += lax.dot_general(
                    score_low, k_rows, TN, preferred_element_type=jnp.float32
                )
                return inner

            def many_tiles(index, inner):
                for part in range(STEP[keys]):
                    key_tile(key_begin + STEP[keys] * index + part, inner)
                return inner

            steps = jnp.maximum(key_end - key_begin, 0) // STEP[keys]
            lax.fori_loop(0, steps, many_tiles, 0)
            lax.fori_loop(key_begin + STEP[keys] * steps, key_end, key_tile, 0)
            if keys != "far":
                for at_row, (h, s) in enumerate(pairs):
                    part = q_acc[tile, at_row * ROWS : (at_row + 1) * ROWS, :] * scaling
                    q_ref[block + s, :, h * HEAD : (h + 1) * HEAD] = part.astype(jnp.bfloat16)
            q_copy(tile).start()
            return carry

        lax.fori_loop(0, tiles, query_tile, 0)
        if keys == "all":
            pltpu.sync_copy(acc, sums_out[0])
        else:
            sums_copy().wait()
            for ref, (begin, size) in zip(sums_out, targets):
                total = acc[begin : begin + size] + sums_ref[begin : begin + size]
                ref[:, 0:HEAD] = (total[:, 0:HEAD] * scaling).astype(ref.dtype)
                ref[:, HEAD : 2 * HEAD] = total[:, HEAD : 2 * HEAD].astype(ref.dtype)
        for tile in range(tiles):
            q_copy(tile).wait()

    q_shape = jax.ShapeDtypeStruct((MEMBERS, ROWS, WIDTH), jnp.bfloat16)
    acc_shape = (WINDOW, pair)
    q_acc_shape = (tiles, H * TQ, HEAD)
    if keys == "all":
        out_shape = [q_shape, jax.ShapeDtypeStruct(acc_shape, jnp.float32)]
        out_specs = [ANY, ANY]
    elif keys == "far":
        out_shape = [jax.ShapeDtypeStruct(q_acc_shape, jnp.float32)]
        out_shape += [jax.ShapeDtypeStruct((size, pair), jnp.bfloat16) for _, size in targets]
        out_specs = [ANY] + [VMEM] * len(targets)
    else:
        out_shape = [q_shape, jax.ShapeDtypeStruct((GROUP, pair), jnp.float32)]
        out_specs = [ANY, VMEM]
    return pl.pallas_call(
        kernel,
        in_specs=[SMEM, SMEM] + [ANY] * (len(operands) - 2),
        out_specs=out_specs,
        out_shape=out_shape,
        scratch_shapes=[
            pltpu.VMEM((MEMBERS, ROWS + STATS, 2 * WIDTH), jnp.bfloat16),
            pltpu.VMEM(q_shape.shape, q_shape.dtype),
            pltpu.VMEM((WINDOW, pair), jnp.bfloat16),
            pltpu.VMEM(acc_shape, jnp.float32),
            pltpu.VMEM(q_acc_shape, jnp.float32),
            pltpu.SemaphoreType.DMA((tiles,)),
            pltpu.SemaphoreType.DMA((4,)),
            pltpu.SemaphoreType.DMA((tiles,)),
            pltpu.VMEM(acc_shape, jnp.float32),
            pltpu.SemaphoreType.DMA,
            pltpu.SemaphoreType.DMA((tiles,)),
        ],
        compiler_params=BIG,
    )(*operands)


def kv_sum(member, near, back1, back2):
    skip = (GROUP - FAR2) // ROWS
    wide = 2 * HEAD

    def kernel(member_ref, near_hbm, back1_hbm, back2_hbm, *rest):
        outs, (near_ref, back1_ref, back2_ref, out_ref, sems) = rest[:MEMBERS], rest[MEMBERS:]

        def inbound(k):
            b = (member_ref[0] + k) % MEMBERS
            cut = pl.ds(pl.multiple_of(b * ROWS, ROWS), ROWS)
            far = pl.ds(pl.multiple_of(jnp.maximum(b - skip, 0) * ROWS, ROWS), ROWS)
            return (
                pltpu.make_async_copy(near_hbm.at[cut], near_ref.at[k], sems.at[0, k]),
                pltpu.make_async_copy(back1_hbm.at[cut], back1_ref.at[k], sems.at[1, k]),
                pltpu.make_async_copy(back2_hbm.at[far], back2_ref.at[k], sems.at[2, k]),
            )

        def outbound(k):
            return pltpu.make_async_copy(out_ref.at[k], outs[k], sems.at[3, k])

        for k in range(MEMBERS):
            for copy in inbound(k):
                copy.start()
        for k in range(MEMBERS):
            for copy in inbound(k):
                copy.wait()
            reached = (member_ref[0] + k) % MEMBERS >= skip
            total = near_ref[k] + back1_ref[k].astype(jnp.float32)
            total = total + jnp.where(reached, back2_ref[k].astype(jnp.float32), 0.0)
            out_ref[k] = total.astype(jnp.bfloat16)
            outbound(k).start()
        for k in range(MEMBERS):
            outbound(k).wait()

    shape = (MEMBERS, ROWS, wide)
    return pl.pallas_call(
        kernel,
        in_specs=[SMEM] + [ANY] * 3,
        out_specs=[ANY] * MEMBERS,
        out_shape=[jax.ShapeDtypeStruct((ROWS, wide), jnp.bfloat16)] * MEMBERS,
        scratch_shapes=[
            pltpu.VMEM(shape, jnp.float32),
            pltpu.VMEM(shape, jnp.bfloat16),
            pltpu.VMEM(shape, jnp.bfloat16),
            pltpu.VMEM(shape, jnp.bfloat16),
            pltpu.SemaphoreType.DMA((4, MEMBERS)),
        ],
        compiler_params=BIG,
        name="kv_sum",
    )(member, near, back1, back2)


def q_unpack(parts):
    def kernel(*refs):
        sources, (out_ref, narrow, wide, arrived, sent) = refs[:CHUNKS], refs[CHUNKS:]
        pieces = [(chunk, b) for chunk in range(CHUNKS) for b in range(MEMBERS)]

        def inbound(chunk, b):
            return pltpu.make_async_copy(
                sources[chunk].at[b], narrow.at[chunk, b], arrived.at[chunk, b]
            )

        def outbound(chunk, b):
            cut = pl.ds((b * CHUNKS + chunk) * WIDTH, WIDTH)
            return pltpu.make_async_copy(
                wide.at[chunk, b], out_ref.at[:, cut], sent.at[chunk, b]
            )

        for piece in pieces:
            inbound(*piece).start()
        for chunk, b in pieces:
            inbound(chunk, b).wait()
            wide[chunk, b] = narrow[chunk, b].astype(jnp.float32)
            outbound(chunk, b).start()
        for piece in pieces:
            outbound(*piece).wait()

    shape = (CHUNKS, MEMBERS, ROWS, WIDTH)
    return pl.pallas_call(
        kernel,
        in_specs=[ANY] * CHUNKS,
        out_specs=ANY,
        out_shape=jax.ShapeDtypeStruct((ROWS, MEMBERS * CHUNKS * WIDTH), jnp.float32),
        scratch_shapes=[
            pltpu.VMEM(shape, jnp.bfloat16),
            pltpu.VMEM(shape, jnp.float32),
            pltpu.SemaphoreType.DMA((CHUNKS, MEMBERS)),
            pltpu.SemaphoreType.DMA((CHUNKS, MEMBERS)),
        ],
        compiler_params=BIG,
        name="q_unpack",
    )(*parts)


def kv_unpack(member, pieces):
    def kernel(member_ref, *rest):
        sources, (k_hbm, v_hbm, both_ref, k_ref, v_ref, sems) = rest[:MEMBERS], rest[MEMBERS:]

        def inbound(k):
            return pltpu.make_async_copy(sources[k], both_ref.at[k], sems.at[0, k])

        def outbound(k):
            head = (member_ref[0] + MEMBERS - k) % MEMBERS
            cut = pl.ds(pl.multiple_of(head * HEAD, HEAD), HEAD)
            return (
                pltpu.make_async_copy(k_ref.at[k], k_hbm.at[:, cut], sems.at[1, k]),
                pltpu.make_async_copy(v_ref.at[k], v_hbm.at[:, cut], sems.at[2, k]),
            )

        for k in range(MEMBERS):
            inbound(k).start()
        for k in range(MEMBERS):
            inbound(k).wait()
            k_ref[k] = both_ref[k, :, 0:HEAD].astype(jnp.float32)
            v_ref[k] = both_ref[k, :, HEAD:].astype(jnp.float32)
            for copy in outbound(k):
                copy.start()
        for k in range(MEMBERS):
            for copy in outbound(k):
                copy.wait()

    shape = jax.ShapeDtypeStruct((ROWS, MEMBERS * HEAD), jnp.float32)
    halves = pltpu.VMEM((MEMBERS, ROWS, HEAD), jnp.float32)
    return pl.pallas_call(
        kernel,
        in_specs=[SMEM] + [ANY] * MEMBERS,
        out_specs=[ANY, ANY],
        out_shape=[shape, shape],
        scratch_shapes=[
            pltpu.VMEM((MEMBERS, ROWS, 2 * HEAD), jnp.bfloat16),
            halves,
            halves,
            pltpu.SemaphoreType.DMA((3, MEMBERS)),
        ],
        compiler_params=BIG,
        name="kv_unpack",
    )(member, *pieces)


def exchange(blocks):
    return lax.all_to_all(blocks, ("core", "head"), split_axis=0, concat_axis=0, tiled=True)


def shifted(block, by):
    count = lax.axis_size("group")
    pairs = [(i, i + by) for i in range(count) if 0 <= i + by < count]
    return lax.ppermute(block, "group", pairs)


def on_device(queries, keys, values, out_rows, output_gradient, log_norm_rows, doc_lengths):
    near = exchange(kv_pack(keys, values)).reshape(GROUP, 2 * HEAD)
    norms = log_norm_rows.T
    rows = []
    for chunk in range(CHUNKS):
        packed = rows_pack(queries, output_gradient, out_rows, norms, chunk)
        rows.append(exchange(packed))
    forwarded = shifted(near[GROUP - FAR2 :], 1)
    far1 = (shifted(near[: GROUP - FAR2], 1), forwarded)
    far2 = shifted(forwarded, 1)
    first_token = (lax.axis_index("group") * GROUP).astype(jnp.int32).reshape(1)
    member = lax.axis_index(("core", "head")).astype(jnp.int32).reshape(1)
    fixed = (doc_lengths, first_token)
    q_part, sums = attention(*fixed, rows[0], far2, far1, near, None, None, "all")
    q_back = [exchange(q_part)]
    q_far, far2_sum, far1_sum = attention(*fixed, rows[1], far2, far1, near, sums, None, "far")
    back1 = shifted(far1_sum, -1)
    back2 = shifted(far2_sum, -2)
    q_part, near_sum = attention(
        *fixed, rows[1], far2, far1, near, sums, q_far, "near"
    )
    q_back.append(exchange(q_part))
    pieces = list(kv_sum(member, near_sum, back1, back2))
    for k in range(1, MEMBERS):
        ring = [(i, (i + k) % MEMBERS) for i in range(MEMBERS)]
        pieces[k] = lax.ppermute(pieces[k], ("core", "head"), ring)
    key_gradient, value_gradient = kv_unpack(member, pieces)
    q_grad = q_unpack(q_back)
    return (q_grad, key_gradient, value_gradient)


def solution(mesh):
    wide, head = mesh.shape["wide"], mesh.shape["head"]
    cores = MEMBERS // head
    finer = Mesh(mesh.devices.reshape(wide // cores, cores, head), ("group", "core", "head"))
    split = P(("group", "core", "head"), None)
    return jax.shard_map(
        on_device,
        mesh=finer,
        in_specs=(split,) * 6 + (P(),),
        out_specs=(split, split, split),
        check_vma=False,
    )
```
